32 devices in a mesh: data: 4 (over x, y), model: 8 (over z, core).
Axes of the slice: x: 2, y: 2, z: 4, core: 2. Of those that a mesh axis runs over, the one named last changes fastest.
Arguments:
- resid_x: bfloat16 [16384, 2048], P('data'), parts along dimension 0
- ln_mean: float32 [16384], P('data'), parts along dimension 0
- ln_rstd: float32 [16384], P('data'), parts along dimension 0
- ln_gain: bfloat16 [2048], replicated
- grad_y: bfloat16 [16384, 2048], P('data'), parts along dimension 0
- w_qkv: bfloat16 [2048, 6144], P(None, 'model')
- w_out: bfloat16 [8, 256, 2048], P('model')
- w_up: bfloat16 [2048, 8192], P(None, 'model')
- w_down: bfloat16 [8192, 2048], P('model')
Outputs:
- output 1: bfloat16 [16384, 2048], P('data'), parts along dimension 0
- output 2: bfloat16 [8192, 6144], P('data', 'model'), parts along dimension 0
- output 3: bfloat16 [32, 256, 2048], P(('data', 'model')), parts along dimension 0
- output 4: bfloat16 [8192, 8192], P('data', 'model'), parts along dimension 0
- output 5: bfloat16 [32768, 2048], P(('data', 'model')), parts along dimension 0
There are 4 independent parts. The reference program is written for one: setup_inputs(seed, part) draws one part's arguments, and reference() takes and returns one part's arrays. A program takes and returns all parts, laid end to end along the dimension named above; an argument that names none is the same for every part.
All inputs are finite; a program needn't handle non-finite values.
Results may differ from the reference program's by a relative error of at most 0.0138052.
Values are sent between devices in bfloat16 or wider.
A program may use at most 1 GiB of HBM per device.

```python
import jax
import jax.numpy as jnp
from jax import lax

TOKENS = 4096
D = 2048
HEADS = 8
FF = 8192

HEAD = D // HEADS
ROT = HEAD // 4
HALF = ROT // 2


def setup_inputs(seed: int = 0, part: int = 0) -> dict:
    part_key = jax.random.fold_in(jax.random.key(seed), part)
    key_x, key_rows, key_off, key_dy = jax.random.split(part_key, 4)
    key_gain, key_qkv, key_out, key_up, key_down = jax.random.split(jax.random.key(seed + 1), 5)
    row_scale = 0.8 * jnp.exp2(jax.random.uniform(key_rows, (TOKENS, 1), jnp.float32, -1.0, 1.0))
    row_offset = 0.5 * jax.random.normal(key_off, (TOKENS, 1), jnp.float32)
    resid_x = (row_scale * jax.random.normal(key_x, (TOKENS, D), jnp.float32) + row_offset).astype(jnp.bfloat16)
    x_f32 = resid_x.astype(jnp.float32)
    ln_mean = jnp.mean(x_f32, axis=1)
    ln_rstd = lax.rsqrt(jnp.mean(jnp.square(x_f32 - ln_mean[:, None]), axis=1) + 1e-5)
    ln_gain = (1.0 + 0.3 * jax.random.normal(key_gain, (D,), jnp.float32)).astype(jnp.bfloat16)
    grad_y = jax.random.normal(key_dy, (TOKENS, D), jnp.float32).astype(jnp.bfloat16)
    fan_d = D ** -0.5
    w_qkv = (1.5 * fan_d * jax.random.normal(key_qkv, (D, 3 * D), jnp.float32)).astype(jnp.bfloat16)
    w_out = (2.0 * fan_d * jax.random.normal(key_out, (HEADS, HEAD, D), jnp.float32)).astype(jnp.bfloat16)
    w_up = (fan_d * jax.random.normal(key_up, (D, FF), jnp.float32)).astype(jnp.bfloat16)
    w_down = (FF ** -0.5 * jax.random.normal(key_down, (FF, D), jnp.float32)).astype(jnp.bfloat16)
    return {"resid_x": resid_x, "ln_mean": ln_mean, "ln_rstd": ln_rstd, "ln_gain": ln_gain, "grad_y": grad_y, "w_qkv": w_qkv, "w_out": w_out, "w_up": w_up, "w_down": w_down}


def rope_tables():
    positions = jnp.arange(TOKENS, dtype=jnp.float32)[:, None]
    inv_freq = jnp.power(10000.0, -2.0 * jnp.arange(HALF, dtype=jnp.float32) / ROT)
    angles = positions * inv_freq[None, :]
    return jnp.cos(angles)[:, None, :], jnp.sin(angles)[:, None, :]


def rotate(vectors, rope_cos, rope_sin):
    first_half = vectors[..., :HALF]
    second_half = vectors[..., HALF:ROT]
    return jnp.concatenate([first_half * rope_cos - second_half * rope_sin, second_half * rope_cos + first_half * rope_sin, vectors[..., ROT:]], axis=-1)


def exact_gelu(pre_act):
    return jax.nn.gelu(pre_act, approximate=False)


def head_pass(operands):
    q_head, k_head, v_head, d_head = operands
    att_scale = HEAD ** -0.5
    scores = jnp.dot(q_head, k_head.T, preferred_element_type=jnp.float32) * att_scale
    causal = jnp.arange(TOKENS)[:, None] >= jnp.arange(TOKENS)[None, :]
    attn_probs = jax.nn.softmax(jnp.where(causal, scores, -1e30), axis=-1)
    probs_bf = attn_probs.astype(jnp.bfloat16)
    attn_out = jnp.dot(probs_bf, v_head, preferred_element_type=jnp.float32).astype(jnp.bfloat16)
    d_probs = jnp.dot(d_head, v_head.T, preferred_element_type=jnp.float32)
    d_values = jnp.dot(probs_bf.T, d_head, preferred_element_type=jnp.float32)
    row_delta = jnp.sum(attn_probs * d_probs, axis=-1, keepdims=True)
    d_scores = (attn_probs * (d_probs - row_delta) * att_scale).astype(jnp.bfloat16)
    d_q_rot = jnp.dot(d_scores, k_head, preferred_element_type=jnp.float32)
    d_k_rot = jnp.dot(d_scores.T, q_head, preferred_element_type=jnp.float32)
    return attn_out, d_q_rot, d_k_rot, d_values


def reference(resid_x, ln_mean, ln_rstd, ln_gain, grad_y, w_qkv, w_out, w_up, w_down):
    x_hat = (resid_x.astype(jnp.float32) - ln_mean[:, None]) * ln_rstd[:, None]
    gain_f32 = ln_gain.astype(jnp.float32)
    normed = (x_hat * gain_f32).astype(jnp.bfloat16)
    qkv_proj = jnp.dot(normed, w_qkv, preferred_element_type=jnp.float32).reshape(TOKENS, HEADS, 3, HEAD)
    rope_cos, rope_sin = rope_tables()
    q_rot = rotate(qkv_proj[:, :, 0, :], rope_cos, rope_sin).astype(jnp.bfloat16)
    k_rot = rotate(qkv_proj[:, :, 1, :], rope_cos, rope_sin).astype(jnp.bfloat16)
    values = qkv_proj[:, :, 2, :].astype(jnp.bfloat16)
    w_out_rows = w_out.reshape(D, D)
    d_attn = jnp.dot(grad_y, w_out_rows.T, preferred_element_type=jnp.float32).astype(jnp.bfloat16).reshape(TOKENS, HEADS, HEAD)
    head_major = (jnp.transpose(q_rot, (1, 0, 2)), jnp.transpose(k_rot, (1, 0, 2)), jnp.transpose(values, (1, 0, 2)), jnp.transpose(d_attn, (1, 0, 2)))
    head_outs, head_dq, head_dk, head_dv = lax.map(head_pass, head_major)
    attn_out = jnp.transpose(head_outs, (1, 0, 2)).reshape(TOKENS, D)
    d_queries = rotate(jnp.transpose(head_dq, (1, 0, 2)), rope_cos, -rope_sin)
    d_keys = rotate(jnp.transpose(head_dk, (1, 0, 2)), rope_cos, -rope_sin)
    d_values = jnp.transpose(head_dv, (1, 0, 2))
    d_qkv = jnp.stack([d_queries, d_keys, d_values], axis=2).astype(jnp.bfloat16).reshape(TOKENS, 3 * D)
    grad_w_qkv = jnp.dot(normed.T, d_qkv, preferred_element_type=jnp.float32).astype(jnp.bfloat16)
    grad_w_out = jnp.dot(attn_out.T, grad_y, preferred_element_type=jnp.float32).astype(jnp.bfloat16).reshape(HEADS, HEAD, D)
    pre_act = jnp.dot(normed, w_up, preferred_element_type=jnp.float32)
    act_out, gelu_vjp = jax.vjp(exact_gelu, pre_act)
    act_bf = act_out.astype(jnp.bfloat16)
    grad_w_down = jnp.dot(act_bf.T, grad_y, preferred_element_type=jnp.float32).astype(jnp.bfloat16)
    d_act = jnp.dot(grad_y, w_down.T, preferred_element_type=jnp.float32)
    d_pre = gelu_vjp(d_act)[0].astype(jnp.bfloat16)
    grad_w_up = jnp.dot(normed.T, d_pre, preferred_element_type=jnp.float32).astype(jnp.bfloat16)
    d_normed = jnp.dot(d_pre, w_up.T, preferred_element_type=jnp.float32) + jnp.dot(d_qkv, w_qkv.T, preferred_element_type=jnp.float32)
    d_hat = d_normed * gain_f32
    mean_d = jnp.mean(d_hat, axis=1, keepdims=True)
    mean_dx = jnp.mean(d_hat * x_hat, axis=1, keepdims=True)
    grad_x = (grad_y.astype(jnp.float32) + ln_rstd[:, None] * (d_hat - mean_d - x_hat * mean_dx)).astype(jnp.bfloat16)
    return (grad_x, grad_w_qkv, grad_w_out, grad_w_up, grad_w_down)
```

```python
import functools

import jax
import jax.numpy as jnp
import numpy as np
from jax import lax
from jax.experimental import pallas as pl
from jax.experimental.pallas import tpu as pltpu
from jax.sharding import PartitionSpec as P

MESH = pl.DeviceIdType.MESH
F32, BF16 = jnp.float32, jnp.bfloat16
ROWS = 256
NEG = -1e30


def mm(a, b):
    return jnp.dot(a, b, preferred_element_type=F32)


def mm_nt(a, b):
    return lax.dot_general(a, b, (((1,), (1,)), ((), ())), preferred_element_type=F32)


def mm_tn(a, b):
    return lax.dot_general(a, b, (((0,), (0,)), ((), ())), preferred_element_type=F32)


def clip(v, hi):
    return jnp.minimum(jnp.maximum(v, 0), hi)


def layer_kernel(dims, x_hbm, dy_hbm, g_ref, cb_ref, sb_ref, co_ref, so_ref, wqkv_hbm, wo_hbm, w1_hbm, w2_hbm,
                 dx_hbm, dwqkv_hbm, dwo_hbm, dw1_hbm, dw2_hbm, n_hbm, g_hbm, da_hbm, dqkv_hbm, o_hbm, zin_hbm, xin_hbm,
                 qbuf, pst, sib_in, zst, xst, lx, ly,
                 sib_s, sib_r, qs_s, z_r, x_r, dxl_s, dxs_s, dxo_s, dxo_r, dxs_r, st_sem, in_sem, w_sem, out_sem, t2_sem):
    T, D, F, H, C = dims
    R = ROWS
    HALF = R // 2
    NB = T // R
    QPC = C // R
    me = lax.axis_index("model")
    core = lax.rem(me, 2)
    z = me // 2
    nbz = z + 1 - 2 * lax.rem(z, 2)
    sibling = z * 2 + 1 - core
    near = nbz * 2 + core
    partner = (3 - z) * 2 + core
    is_mid = (z == 1) | (z == 2)
    is_out = (z == 0) | (z == 3)

    barrier = pltpu.get_barrier_semaphore()
    pl.semaphore_signal(barrier, inc=1, device_id={"model": sibling}, device_id_type=MESH)
    pl.semaphore_signal(barrier, inc=1, device_id={"model": near}, device_id_type=MESH)

    @pl.when(is_mid)
    def _():
        pl.semaphore_signal(barrier, inc=1, device_id={"model": partner}, device_id_type=MESH)
        pl.semaphore_wait(barrier, 3)

    @pl.when(is_out)
    def _():
        pl.semaphore_wait(barrier, 2)

    def rows_of(t, c):
        return pl.ds(pl.multiple_of((NB - 1 - t) * R + c * HALF, HALF), HALF)

    def sib_copy(t):
        s = lax.rem(t, 2)
        return pltpu.make_async_remote_copy(src_ref=pst.at[pl.ds(pl.multiple_of((1 - core) * HALF, HALF), HALF)], dst_ref=sib_in.at[s],
                                            send_sem=sib_s.at[s], recv_sem=sib_r.at[s], device_id={"model": sibling}, device_id_type=MESH)

    def q_copy(t):
        return pltpu.make_async_remote_copy(src_ref=qbuf.at[t], dst_ref=zin_hbm.at[t], send_sem=qs_s.at[t], recv_sem=z_r.at[t],
                                            device_id={"model": near}, device_id_type=MESH)

    def x_copy(t):
        return pltpu.make_async_remote_copy(src_ref=qbuf.at[t], dst_ref=xin_hbm.at[t], send_sem=qs_s.at[t], recv_sem=x_r.at[t],
                                            device_id={"model": partner}, device_id_type=MESH)

    def dx_local(t):
        return pltpu.make_async_copy(qbuf.at[t], dx_hbm.at[rows_of(t, core)], dxl_s.at[t])

    def dx_sib(t):
        return pltpu.make_async_remote_copy(src_ref=qbuf.at[t], dst_ref=dx_hbm.at[rows_of(t, core)], send_sem=dxs_s.at[t], recv_sem=dxs_r.at[t],
                                            device_id={"model": sibling}, device_id_type=MESH)

    def dx_out(t):
        return pltpu.make_async_remote_copy(src_ref=qbuf.at[t], dst_ref=dx_hbm.at[rows_of(t, core)], send_sem=dxo_s.at[t], recv_sem=dxo_r.at[t],
                                            device_id={"model": near}, device_id_type=MESH)

    def dx_fwd(t):
        return pltpu.make_async_remote_copy(src_ref=dx_hbm.at[rows_of(t, core)], dst_ref=dx_hbm.at[rows_of(t, core)], send_sem=dxs_s.at[t],
                                            recv_sem=dxs_r.at[t], device_id={"model": sibling}, device_id_type=MESH)

    def z_load(t):
        return pltpu.make_async_copy(zin_hbm.at[t], zst, st_sem.at[0])

    def x_load(t):
        return pltpu.make_async_copy(xin_hbm.at[t], xst, st_sem.at[1])

    def lx_load(t):
        return pltpu.make_async_copy(x_hbm.at[rows_of(t, core)], lx, st_sem.at[2])

    def ly_load(t):
        return pltpu.make_async_copy(dy_hbm.at[rows_of(t, core)], ly, st_sem.at[3])

    def pair_sum(t):
        cp = sib_copy(t)
        cp.wait_send()
        cp.wait_recv()
        own = pst[pl.ds(pl.multiple_of(core * HALF, HALF), HALF), :].astype(F32)
        qbuf[t] = (own + sib_in[lax.rem(t, 2)].astype(F32)).astype(BF16)

        @pl.when(is_out)
        def _():
            q_copy(t).start()

    def e3_fetch(t):
        q_copy(t).wait_recv()
        z_load(t).start()

    def e3_process(t):
        z_load(t).wait()
        qbuf[t] = (qbuf[t].astype(F32) + zst[...].astype(F32)).astype(BF16)
        x_copy(t).start()

    def e4_fetch(t):
        x_copy(t).wait_recv()
        x_load(t).start()
        lx_load(t).start()
        ly_load(t).start()

    def e4_process(t):
        x_load(t).wait()
        lx_load(t).wait()
        ly_load(t).wait()
        x_copy(t).wait_send()
        xv = lx[...].astype(F32)
        mean = jnp.sum(xv, axis=1, keepdims=True) * (1.0 / D)
        xc = xv - mean
        rstd = lax.rsqrt(jnp.sum(xc * xc, axis=1, keepdims=True) * (1.0 / D) + 1e-5)
        xh = xc * rstd
        d = (qbuf[t].astype(F32) + xst[...].astype(F32)) * g_ref[...]
        md = jnp.sum(d, axis=1, keepdims=True) * (1.0 / D)
        mdx = jnp.sum(d * xh, axis=1, keepdims=True) * (1.0 / D)
        qbuf[t] = (ly[...].astype(F32) + rstd * (d - md - xh * mdx)).astype(BF16)
        dx_out(t).start()
        dx_sib(t).start()
        dx_local(t).start()

    def e5(t):
        dx_out(t).wait_recv()
        dx_fwd(t).start()

    def service_fetch(lo3, hi3, lo4, hi4, lo5, hi5):
        @pl.when(is_mid & (hi3 > lo3))
        def _():
            e3_fetch(lo3)

        @pl.when(is_mid & (hi4 > lo4))
        def _():
            e4_fetch(lo4)

        @pl.when(is_out & (hi5 > lo5))
        def _():
            e5(lo5)

    def service_process(lo3, hi3, lo4, hi4, lo5, hi5):
        @pl.when(is_mid & (hi3 > lo3))
        def _():
            e3_process(lo3)

        @pl.when(is_mid & (hi4 > lo4))
        def _():
            e4_process(lo4)

    def n_phase1(u, lag):
        return clip((5 * (u - lag) + 5) // 6, NB)

    LAG3, LAG4, LAG5 = 2, 4, 6

    def ticks1(u):
        return (n_phase1(u - 1, LAG3), n_phase1(u, LAG3), n_phase1(u - 1, LAG4), n_phase1(u, LAG4), n_phase1(u - 1, LAG5), n_phase1(u, LAG5))

    def n_phase2(w, lag):
        return jnp.minimum(n_phase1(NB - 1, lag) + (2 * (w + 1)) // 5, NB)

    def ticks2(w):
        return (n_phase2(w - 1, LAG3), n_phase2(w, LAG3), n_phase2(w - 1, LAG4), n_phase2(w, LAG4), n_phase2(w - 1, LAG5), n_phase2(w, LAG5))

    def rope_of(i):
        cb, sb = cb_ref[pl.ds(i, 1), :], sb_ref[pl.ds(i, 1), :]
        co, so = co_ref[...], so_ref[...]
        return cb * co - sb * so, sb * co + cb * so

    def rope(x, cosf, sinf):
        x0 = x[:, :128]
        lane = lax.broadcasted_iota(jnp.int32, x0.shape, 1)
        other = jnp.where(lane < H // 8, pltpu.roll(x0, 128 - H // 8, 1), pltpu.roll(x0, H // 8, 1))
        return jnp.concatenate([x0 * cosf + other * sinf, x[:, 128:]], axis=1)

    def attention_phase(kv, kT, vv, vT, dk, dv, es, dps, w1, w2, wqkv, wo, nbuf, ybuf, gst, dast, dqkvst, ost, qs, qT, do, doT, oT, dqT, msc):
        w_loads = [pltpu.make_async_copy(s, d_, w_sem.at[k]) for k, (s, d_) in enumerate(((wqkv_hbm, wqkv), (wo_hbm, wo), (w1_hbm, w1), (w2_hbm, w2)))]

        def blk(i):
            return pl.ds(pl.multiple_of(i * R, R), R)

        def x_in(b):
            return pltpu.make_async_copy(x_hbm.at[blk(b)], ybuf.at[lax.rem(b, 2)], in_sem.at[0, lax.rem(b, 2)])

        def n_out(b):
            return pltpu.make_async_copy(nbuf.at[lax.rem(b, 2)], n_hbm.at[blk(b)], out_sem.at[0, lax.rem(b, 2)])

        w_loads[0].start()
        x_in(0).start()
        for w in w_loads[1:]:
            w.start()
        dk[...] = jnp.zeros_like(dk)
        dv[...] = jnp.zeros_like(dv)
        w_loads[0].wait()

        @pl.loop(0, NB)
        def _(b):
            slot = lax.rem(b, 2)
            x_in(b).wait()

            @pl.when(b + 1 < NB)
            def _():
                x_in(b + 1).start()

            @pl.when(b >= 2)
            def _():
                n_out(b - 2).wait()

            xv = ybuf[slot].astype(F32)
            mean = jnp.sum(xv, axis=1, keepdims=True) * (1.0 / D)
            xc = xv - mean
            rstd = lax.rsqrt(jnp.sum(xc * xc, axis=1, keepdims=True) * (1.0 / D) + 1e-5)
            nbuf[slot] = ((xc * rstd) * g_ref[...]).astype(BF16)
            n_out(b).start()
            kvp = mm(nbuf[slot], wqkv[:, H:])
            cosf, sinf = rope_of(b)
            kf = rope(kvp[:, :H], cosf, sinf)
            vf = kvp[:, H:]
            kv[blk(b), :] = kf.astype(BF16)
            vv[blk(b), :] = vf.astype(BF16)
            kT[:, blk(b)] = kf.T.astype(BF16)
            vT[:, blk(b)] = vf.T.astype(BF16)

        n_out(NB - 2).wait()
        n_out(NB - 1).wait()

        def n_in(t):
            return pltpu.make_async_copy(n_hbm.at[blk(NB - 1 - t)], nbuf.at[lax.rem(t, 2)], in_sem.at[1, lax.rem(t, 2)])

        def y_in(t):
            return pltpu.make_async_copy(dy_hbm.at[blk(NB - 1 - t)], ybuf.at[lax.rem(t, 2)], in_sem.at[0, lax.rem(t, 2)])

        def outs(t):
            s, i = lax.rem(t, 2), NB - 1 - t
            return [pltpu.make_async_copy(gst.at[s], g_hbm.at[blk(i)], out_sem.at[0, s]),
                    pltpu.make_async_copy(dast.at[s], da_hbm.at[blk(i)], out_sem.at[1, s]),
                    pltpu.make_async_copy(dqkvst.at[s], dqkv_hbm.at[blk(i)], out_sem.at[2, s]),
                    pltpu.make_async_copy(ost.at[s], o_hbm.at[blk(i)], out_sem.at[3, s])]

        n_in(0).start()
        y_in(0).start()
        for w in w_loads[1:]:
            w.wait()

        @pl.loop(0, NB)
        def _(t):
            slot = lax.rem(t, 2)
            i = NB - 1 - t
            n_in(t).wait()
            y_in(t).wait()

            @pl.when(t + 1 < NB)
            def _():
                n_in(t + 1).start()
                y_in(t + 1).start()

            @pl.when(t >= 2)
            def _():
                for cp in outs(t - 2):
                    cp.wait()

            service_fetch(*ticks1(t))

            FT = min(512, F)
            for f in range(0, F, FT):
                a = mm(nbuf[slot], w1[:, f:f + FT])
                da = mm_nt(ybuf[slot], w2[f:f + FT, :])
                phi = 0.5 + 0.5 * lax.erf(a * 0.7071067811865476)
                gst[slot, :, f:f + FT] = (a * phi).astype(BF16)
                dast[slot, :, f:f + FT] = (da * (phi + a * (0.3989422804014327 * jnp.exp(-0.5 * (a * a))))).astype(BF16)
            for cp in outs(t)[:2]:
                cp.start()

            @pl.when(t > 0)
            def _():
                pair_sum(t - 1)

            service_process(*ticks1(t))

            cosf, sinf = rope_of(i)
            qf = rope(mm(nbuf[slot], wqkv[:, :H]), cosf, sinf).astype(BF16).astype(F32) * (H ** -0.5)
            qs[...] = qf.astype(BF16)
            qT[...] = qf.T.astype(BF16)
            dof = mm_nt(ybuf[slot], wo[...])
            do[...] = dof.astype(BF16)
            doT[...] = dof.T.astype(BF16)
            nfull = i // QPC

            def chunk(j):
                return pl.ds(pl.multiple_of(j * C, C), C)

            def pass_a(j, carry, masked):
                m, l, dl = carry
                st = mm(kv[chunk(j), :], qT[...])
                if masked:
                    key = j * C + lax.broadcasted_iota(jnp.int32, st.shape, 0)
                    query = i * R + lax.broadcasted_iota(jnp.int32, st.shape, 1)
                    st = jnp.where(key <= query, st, NEG)
                dp = mm(vv[chunk(j), :], doT[...])
                m_new = jnp.maximum(m, jnp.max(st, axis=0, keepdims=True))
                alpha = jnp.exp(m - m_new)
                e = jnp.exp(st - m_new)
                es[chunk(j), :] = e
                dps[chunk(j), :] = dp
                msc[pl.ds(j, 1), :] = m_new
                return m_new, l * alpha + jnp.sum(e, axis=0, keepdims=True), dl * alpha + jnp.sum(e * dp, axis=0, keepdims=True)

            init = (jnp.full((1, R), NEG, F32), jnp.zeros((1, R), F32), jnp.zeros((1, R), F32))
            carry = lax.fori_loop(0, nfull, functools.partial(pass_a, masked=False), init)
            m, l, dl = pass_a(nfull, carry, True)
            inv_l = 1.0 / l
            delta = dl * inv_l
            oT[...] = jnp.zeros_like(oT)
            dqT[...] = jnp.zeros_like(dqT)

            @pl.loop(0, nfull + 1)
            def _(j):
                p = es[chunk(j), :] * (jnp.exp(msc[pl.ds(j, 1), :] - m) * inv_l)
                pb = p.astype(BF16)
                ds = (p * (dps[chunk(j), :] - delta)).astype(BF16)
                oT[...] += mm(vT[:, chunk(j)], pb)
                dqT[...] += mm(kT[:, chunk(j)], ds)
                dv[chunk(j), :] += mm(pb, do[...])
                dk[chunk(j), :] += mm(ds, qs[...])

            ost[slot] = oT[...].T.astype(BF16)
            dqkvst[slot, :, :H] = rope(dqT[...].T * (H ** -0.5), cosf, -sinf).astype(BF16)
            dqkvst[slot, :, H:2 * H] = rope(dk[blk(i), :], cosf, -sinf).astype(BF16)
            dqkvst[slot, :, 2 * H:] = dv[blk(i), :].astype(BF16)
            for cp in outs(t)[2:]:
                cp.start()

            DT = min(512, D)
            for c in range(0, D, DT):
                pst[:, c:c + DT] = (mm_nt(dast[slot], w1[c:c + DT, :]) + mm_nt(dqkvst[slot], wqkv[c:c + DT, :])).astype(BF16)
            sib_copy(t).start()

        for t in (NB - 2, NB - 1):
            for cp in outs(t):
                cp.wait()

    pl.run_scoped(
        attention_phase,
        pltpu.VMEM((T, H), BF16), pltpu.VMEM((H, T), BF16), pltpu.VMEM((T, H), BF16), pltpu.VMEM((H, T), BF16),
        pltpu.VMEM((T, H), F32), pltpu.VMEM((T, H), F32), pltpu.VMEM((T, R), F32), pltpu.VMEM((T, R), F32),
        pltpu.VMEM((D, F), BF16), pltpu.VMEM((F, D), BF16), pltpu.VMEM((D, 3 * H), BF16), pltpu.VMEM((H, D), BF16),
        pltpu.VMEM((2, R, D), BF16), pltpu.VMEM((2, R, D), BF16), pltpu.VMEM((2, R, F), BF16), pltpu.VMEM((2, R, F), BF16),
        pltpu.VMEM((2, R, 3 * H), BF16), pltpu.VMEM((2, R, H), BF16),
        pltpu.VMEM((R, H), BF16), pltpu.VMEM((H, R), BF16), pltpu.VMEM((R, H), BF16), pltpu.VMEM((H, R), BF16),
        pltpu.VMEM((H, R), F32), pltpu.VMEM((H, R), F32), pltpu.VMEM((8, R), F32))

    NT1, NT2 = D // H, F // H

    def weight_phase(da, dqkv, dy, nt, w1st, wqst, w2st):
        loads = [pltpu.make_async_copy(s, d_, w_sem.at[k]) for k, (s, d_) in enumerate(((da_hbm, da), (dqkv_hbm, dqkv), (dy_hbm, dy)))]

        def cols(m):
            return pl.ds(pl.multiple_of(m * H, H), H)

        def nt_in(m):
            return pltpu.make_async_copy(n_hbm.at[:, cols(m)], nt.at[lax.rem(m, 2)], t2_sem.at[0, lax.rem(m, 2)])

        def g_in(m):
            return pltpu.make_async_copy(g_hbm.at[:, cols(m)], nt.at[lax.rem(m, 2)], t2_sem.at[0, lax.rem(m, 2)])

        def o_in():
            return pltpu.make_async_copy(o_hbm, nt.at[NT2 % 2], t2_sem.at[0, NT2 % 2])

        def out1(m):
            s = lax.rem(m, 2)
            return [pltpu.make_async_copy(w1st.at[s], dw1_hbm.at[cols(m)], t2_sem.at[1, s]),
                    pltpu.make_async_copy(wqst.at[s], dwqkv_hbm.at[cols(m)], t2_sem.at[2, s])]

        def out2(m):
            return pltpu.make_async_copy(w2st.at[lax.rem(m, 2)], dw2_hbm.at[cols(m)], t2_sem.at[1, lax.rem(m, 2)])

        def out3():
            return pltpu.make_async_copy(w2st.at[NT2 % 2], dwo_hbm, t2_sem.at[1, NT2 % 2])

        loads[0].start()
        nt_in(0).start()
        loads[1].start()
        loads[2].start()
        pair_sum(NB - 1)
        loads[0].wait()
        loads[1].wait()

        @pl.loop(0, NT1)
        def _(m):
            s = lax.rem(m, 2)
            nt_in(m).wait()

            @pl.when(m + 1 < NT1)
            def _():
                nt_in(m + 1).start()

            @pl.when(m + 1 == NT1)
            def _():
                g_in(0).start()

            @pl.when(m >= 2)
            def _():
                for cp in out1(m - 2):
                    cp.wait()

            service_fetch(*ticks2(m))
            w1st[s] = mm_tn(nt[s], da[...]).astype(BF16)
            wqst[s] = mm_tn(nt[s], dqkv[...]).astype(BF16)
            for cp in out1(m):
                cp.start()
            service_process(*ticks2(m))

        for m in (NT1 - 2, NT1 - 1):
            for cp in out1(m):
                cp.wait()
        loads[2].wait()

        @pl.loop(0, NT2)
        def _(m):
            s = lax.rem(m, 2)
            g_in(m).wait()

            @pl.when(m + 1 < NT2)
            def _():
                g_in(m + 1).start()

            @pl.when(m + 1 == NT2)
            def _():
                o_in().start()

            @pl.when(m >= 2)
            def _():
                out2(m - 2).wait()

            service_fetch(*ticks2(NT1 + m))
            w2st[s] = mm_tn(nt[s], dy[...]).astype(BF16)
            out2(m).start()
            service_process(*ticks2(NT1 + m))

        o_in().wait()
        out2(NT2 - 2).wait()
        service_fetch(*ticks2(NT1 + NT2))
        w2st[NT2 % 2] = mm_tn(nt[NT2 % 2], dy[...]).astype(BF16)
        out3().start()
        service_process(*ticks2(NT1 + NT2))
        out2(NT2 - 1).wait()
        out3().wait()

    pl.run_scoped(
        weight_phase,
        pltpu.VMEM((T, F), BF16), pltpu.VMEM((T, 3 * H), BF16), pltpu.VMEM((T, D), BF16), pltpu.VMEM((2, T, H), BF16),
        pltpu.VMEM((2, H, F), BF16), pltpu.VMEM((2, H, 3 * H), BF16), pltpu.VMEM((2, H, D), BF16))

    WL = NT1 + NT2
    l3, l4, l5 = n_phase2(WL, LAG3), n_phase2(WL, LAG4), n_phase2(WL, LAG5)

    @pl.when(is_mid)
    def _():
        @pl.loop(0, NB - l4)
        def _(k):
            @pl.when(l3 + k < NB)
            def _():
                e3_fetch(l3 + k)
                e3_process(l3 + k)

            e4_fetch(l4 + k)
            e4_process(l4 + k)

        @pl.loop(0, NB)
        def _(t):
            dx_local(t).wait()
            dx_sib(t).wait_send()
            dx_out(t).wait_send()
            dx_sib(t).wait_recv()

    @pl.when(is_out)
    def _():
        @pl.loop(l5, NB)
        def _(t):
            e5(t)

        @pl.loop(0, NB)
        def _(t):
            q_copy(t).wait_send()
            dx_fwd(t).wait_send()
            dx_fwd(t).wait_recv()


def rope_tables(blocks, head_dim):
    rot = head_dim // 4
    half = rot // 2
    inv_freq = np.power(np.float32(10000.0), (-2.0 * np.arange(half, dtype=np.float32) / rot).astype(np.float32)).astype(np.float64)
    freq = np.zeros((1, 128))
    freq[0, :half], freq[0, half:rot] = -inv_freq, inv_freq
    at = np.arange(blocks)[:, None] * ROWS * freq
    off = np.arange(ROWS)[:, None] * freq
    return [np.asarray(t, np.float32) for t in (np.cos(at), np.sin(at), np.cos(off), np.sin(off))]


def solution(mesh):
    def device_step(resid_x, ln_mean, ln_rstd, ln_gain, grad_y, w_qkv, w_out, w_up, w_down):
        T, D = resid_x.shape
        F = w_up.shape[1]
        H = w_out.shape[1]
        NB = T // ROWS
        HALF = ROWS // 2
        C = min(1024, T)
        tabs = [jnp.asarray(t) for t in rope_tables(NB, H)]
        any_spec = pl.BlockSpec(memory_space=pl.ANY)
        vmem = pl.BlockSpec(memory_space=pltpu.VMEM)
        sds = lambda *s: jax.ShapeDtypeStruct(s, BF16)
        outs = pl.pallas_call(
            functools.partial(layer_kernel, (T, D, F, H, C)),
            name="layer_backward",
            out_shape=[sds(T, D), sds(D, 3 * H), sds(H, D), sds(D, F), sds(F, D),
                       sds(T, D), sds(T, F), sds(T, F), sds(T, 3 * H), sds(T, H), sds(NB, HALF, D), sds(NB, HALF, D)],
            in_specs=[any_spec, any_spec, vmem, vmem, vmem, vmem, vmem, any_spec, any_spec, any_spec, any_spec],
            out_specs=[any_spec] * 12,
            scratch_shapes=[
                pltpu.VMEM((NB, HALF, D), BF16), pltpu.VMEM((ROWS, D), BF16), pltpu.VMEM((2, HALF, D), BF16),
                pltpu.VMEM((HALF, D), BF16), pltpu.VMEM((HALF, D), BF16), pltpu.VMEM((HALF, D), BF16), pltpu.VMEM((HALF, D), BF16),
                pltpu.SemaphoreType.DMA((2,)), pltpu.SemaphoreType.DMA((2,))]
            + [pltpu.SemaphoreType.DMA((NB,))] * 8
            + [pltpu.SemaphoreType.DMA((4,)), pltpu.SemaphoreType.DMA((2, 2)), pltpu.SemaphoreType.DMA((4,)), pltpu.SemaphoreType.DMA((4, 2)),
               pltpu.SemaphoreType.DMA((3, 2))],
            compiler_params=pltpu.CompilerParams(collective_id=0, has_side_effects=True, vmem_limit_bytes=67043328),
        )(resid_x, grad_y, ln_gain.astype(F32).reshape(1, D), *tabs, w_qkv, w_out.reshape(H, D), w_up, w_down)
        grad_x, grad_w_qkv, grad_w_out, grad_w_up, grad_w_down = outs[:5]
        return grad_x, grad_w_qkv, grad_w_out.reshape(1, H, D), grad_w_up, grad_w_down

    in_specs = (P("data", None), P("data"), P("data"), P(None), P("data", None), P(None, "model"), P("model", None, None), P(None, "model"), P("model", None))
    out_specs = (P("data", None), P("data", "model"), P(("data", "model"), None, None), P("data", "model"), P(("data", "model"), None))
    return jax.shard_map(device_step, mesh=mesh, in_specs=in_specs, out_specs=out_specs, check_vma=False)
```

```python
import functools

import jax
import jax.numpy as jnp
import numpy as np
from jax import lax
from jax.experimental import pallas as pl
from jax.experimental.pallas import tpu as pltpu
from jax.sharding import PartitionSpec as P

MESH = pl.DeviceIdType.MESH
F32, BF16 = jnp.float32, jnp.bfloat16
ROWS = 256
NEG = -1e30


def mm(a, b):
    return jnp.dot(a, b, preferred_element_type=F32)


def mm_nt(a, b):
    return lax.dot_general(a, b, (((1,), (1,)), ((), ())), preferred_element_type=F32)


def mm_tn(a, b):
    return lax.dot_general(a, b, (((0,), (0,)), ((), ())), preferred_element_type=F32)


def clip(v, hi):
    return jnp.minimum(jnp.maximum(v, 0), hi)


def layer_kernel(dims, plan, x_hbm, dy_hbm, g_ref, mean_ref, rstd_ref, cb_ref, sb_ref, co_ref, so_ref, wqkv_hbm, wo_hbm, w1_hbm, w2_hbm,
                 dx_hbm, dwqkv_hbm, dwo_hbm, dw1_hbm, dw2_hbm, n_hbm, g_hbm, da_hbm, dqkv_hbm, o_hbm, zin_hbm, xin_hbm,
                 qbuf, pst, sib_in, zst, xst, lx, ly,
                 sib_s, sib_r, qs_s, z_r, x_r, dxl_s, dxs_s, dxo_s, dxo_r, dxs_r, st_sem, in_sem, w_sem, out_sem, t2_sem):
    T, D, F, H, C = dims
    R = ROWS
    HALF = R // 2
    PART = HALF // 2
    NB = T // R
    NS = 2 * NB
    QPC = C // R
    me = lax.axis_index("model")
    core = lax.rem(me, 2)
    z = me // 2
    nbz = z + 1 - 2 * lax.rem(z, 2)
    sibling = z * 2 + 1 - core
    near = nbz * 2 + core
    partner = (3 - z) * 2 + core
    is_mid = (z == 1) | (z == 2)
    is_out = (z == 0) | (z == 3)

    barrier = pltpu.get_barrier_semaphore()
    pl.semaphore_signal(barrier, inc=1, device_id={"model": sibling}, device_id_type=MESH)
    pl.semaphore_signal(barrier, inc=1, device_id={"model": near}, device_id_type=MESH)

    @pl.when(is_mid)
    def _():
        pl.semaphore_signal(barrier, inc=1, device_id={"model": partner}, device_id_type=MESH)
        pl.semaphore_wait(barrier, 3)

    @pl.when(is_out)
    def _():
        pl.semaphore_wait(barrier, 2)

    def rows_of(t, c):
        return pl.ds(pl.multiple_of((NB - 1 - t // 2) * R + c * HALF + lax.rem(t, 2) * PART, PART), PART)

    def sib_copy(t):
        s = lax.rem(t, 2)
        return pltpu.make_async_remote_copy(src_ref=pst.at[pl.ds(pl.multiple_of((1 - core) * HALF, HALF), HALF)], dst_ref=sib_in.at[s],
                                            send_sem=sib_s.at[s], recv_sem=sib_r.at[s], device_id={"model": sibling}, device_id_type=MESH)

    def q_copy(t):
        return pltpu.make_async_remote_copy(src_ref=qbuf.at[t], dst_ref=zin_hbm.at[t], send_sem=qs_s.at[t], recv_sem=z_r.at[t],
                                            device_id={"model": near}, device_id_type=MESH)

    def x_copy(t):
        return pltpu.make_async_remote_copy(src_ref=qbuf.at[t], dst_ref=xin_hbm.at[t], send_sem=qs_s.at[t], recv_sem=x_r.at[t],
                                            device_id={"model": partner}, device_id_type=MESH)

    def dx_local(t):
        return pltpu.make_async_copy(qbuf.at[t], dx_hbm.at[rows_of(t, core)], dxl_s.at[t])

    def dx_sib(t):
        return pltpu.make_async_remote_copy(src_ref=qbuf.at[t], dst_ref=dx_hbm.at[rows_of(t, core)], send_sem=dxs_s.at[t], recv_sem=dxs_r.at[t],
                                            device_id={"model": sibling}, device_id_type=MESH)

    def dx_out(t):
        return pltpu.make_async_remote_copy(src_ref=qbuf.at[t], dst_ref=dx_hbm.at[rows_of(t, core)], send_sem=dxo_s.at[t], recv_sem=dxo_r.at[t],
                                            device_id={"model": near}, device_id_type=MESH)

    def dx_fwd(t):
        return pltpu.make_async_remote_copy(src_ref=dx_hbm.at[rows_of(t, core)], dst_ref=dx_hbm.at[rows_of(t, core)], send_sem=dxs_s.at[t],
                                            recv_sem=dxs_r.at[t], device_id={"model": sibling}, device_id_type=MESH)

    def z_load(t):
        return pltpu.make_async_copy(zin_hbm.at[t], zst, st_sem.at[0])

    def x_load(t):
        return pltpu.make_async_copy(xin_hbm.at[t], xst, st_sem.at[1])

    def lx_load(t):
        return pltpu.make_async_copy(x_hbm.at[rows_of(t, core)], lx, st_sem.at[2])

    def ly_load(t):
        return pltpu.make_async_copy(dy_hbm.at[rows_of(t, core)], ly, st_sem.at[3])

    def pair_sum(t):
        cp = sib_copy(t)
        cp.wait_send()
        cp.wait_recv()
        for h in range(2):
            own = pst[pl.ds(pl.multiple_of(core * HALF + h * PART, PART), PART), :].astype(F32)
            qbuf[2 * t + h] = (own + sib_in[lax.rem(t, 2), h * PART:(h + 1) * PART, :].astype(F32)).astype(BF16)

            @pl.when(is_out)
            def _(h=h):
                q_copy(2 * t + h).start()

    def e3_fetch(t):
        q_copy(t).wait_recv()
        z_load(t).start()

    def e3_process(t):
        z_load(t).wait()
        qbuf[t] = (qbuf[t].astype(F32) + zst[...].astype(F32)).astype(BF16)
        x_copy(t).start()

    def e4_fetch(t):
        x_copy(t).wait_recv()
        x_load(t).start()
        lx_load(t).start()
        ly_load(t).start()

    def e4_process(t):
        x_load(t).wait()
        lx_load(t).wait()
        ly_load(t).wait()
        x_copy(t).wait_send()
        mean, rstd = row_stats(NB - 1 - t // 2, core * 2 + lax.rem(t, 2))
        xh = (lx[...].astype(F32) - mean) * rstd
        d = (qbuf[t].astype(F32) + xst[...].astype(F32)) * g_ref[...]
        md = jnp.sum(d, axis=1, keepdims=True) * (1.0 / D)
        mdx = jnp.sum(d * xh, axis=1, keepdims=True) * (1.0 / D)
        qbuf[t] = (ly[...].astype(F32) + rstd * (d - md - xh * mdx)).astype(BF16)
        dx_out(t).start()
        dx_sib(t).start()
        dx_local(t).start()

    def e5(t):
        dx_out(t).wait_recv()
        dx_fwd(t).start()

    def lookup(table, k):
        v = jnp.int32(table[0])
        for at in range(1, len(table)):
            v = jnp.where(k == at, table[at], v)
        return v

    def service_points(table, k):
        start, fire = lookup(table[0], k), lookup(table[1], k)
        c = [start % 64, (start // 64) % 64, (start // 4096) % 64]
        pend = [(start // 262144) % 2, (start // 524288) % 2]
        points = []
        for p in range(table[2]):
            f = [(fire // 2 ** (3 * p + step)) % 2 for step in range(3)]
            points.append((list(c), list(pend), f))
            c = [a + b for a, b in zip(c, f)]
            pend = f[:2]
        return points

    def service(point):
        c, pend, f = point

        @pl.when(is_mid & (pend[0] > 0))
        def _():
            e3_process(c[0] - 1)

        @pl.when(is_mid & (f[0] > 0))
        def _():
            e3_fetch(c[0])

        @pl.when(is_mid & (pend[1] > 0))
        def _():
            e4_process(c[1] - 1)

        @pl.when(is_mid & (f[1] > 0))
        def _():
            e4_fetch(c[1])

        @pl.when(is_out & (f[2] > 0))
        def _():
            e5(c[2])

    def row_stats(i, part=None):
        out = []
        for ref in (mean_ref, rstd_ref):
            row = ref[pl.ds(i, 1), :]
            if part is None:
                col = jnp.broadcast_to(row, (128, R)).T
            else:
                row = jnp.where(part >= 2, row[:, HALF:], row[:, :HALF])
                col = jnp.broadcast_to(row, (128, HALF)).T
                col = jnp.where(lax.rem(part, 2) == 0, col[:PART], col[PART:])
            out.append(jnp.concatenate([col] * (D // 128), axis=1))
        return out

    def rope_of(i):
        cb, sb = cb_ref[pl.ds(i, 1), :], sb_ref[pl.ds(i, 1), :]
        co, so = co_ref[...], so_ref[...]
        return cb * co - sb * so, sb * co + cb * so

    def rope(x, cosf, sinf):
        x0 = x[:, :128]
        lane = lax.broadcasted_iota(jnp.int32, x0.shape, 1)
        other = jnp.where(lane < H // 8, pltpu.roll(x0, 128 - H // 8, 1), pltpu.roll(x0, H // 8, 1))
        return jnp.concatenate([x0 * cosf + other * sinf, x[:, 128:]], axis=1)

    def attention_phase(kv, kT, vv, vT, dk, dv, es, dps, w1, w2, wqkv, wo, nbuf, ybuf, gst, dast, dqkvst, ost, qs, qT, do, doT, oT, dqT, msc):
        w_loads = [pltpu.make_async_copy(s, d_, w_sem.at[k]) for k, (s, d_) in enumerate(((wqkv_hbm, wqkv), (wo_hbm, wo), (w1_hbm, w1), (w2_hbm, w2)))]

        def blk(i):
            return pl.ds(pl.multiple_of(i * R, R), R)

        def x_in(b):
            return pltpu.make_async_copy(x_hbm.at[blk(b)], ybuf.at[lax.rem(b + 1, 2)], in_sem.at[0, lax.rem(b + 1, 2)])

        def n_out(b):
            return pltpu.make_async_copy(nbuf.at[lax.rem(b + 1, 2)], n_hbm.at[blk(b)], out_sem.at[0, lax.rem(b + 1, 2)])

        def n_in(t):
            return pltpu.make_async_copy(n_hbm.at[blk(NB - 1 - t)], nbuf.at[lax.rem(t, 2)], in_sem.at[1, lax.rem(t, 2)])

        def y_in(t):
            return pltpu.make_async_copy(dy_hbm.at[blk(NB - 1 - t)], ybuf.at[lax.rem(t + 1, 2)], in_sem.at[0, lax.rem(t + 1, 2)])

        w_loads[0].start()
        x_in(0).start()
        for w in w_loads[1:]:
            w.start()
        dk[...] = jnp.zeros_like(dk)
        dv[...] = jnp.zeros_like(dv)

        def normed(b):
            slot = lax.rem(b + 1, 2)
            mean, rstd = row_stats(b)
            nbuf[slot] = (((ybuf[slot].astype(F32) - mean) * rstd) * g_ref[...]).astype(BF16)

        def keys_values(b):
            kvp = mm(nbuf[lax.rem(b + 1, 2)], wqkv[:, H:])
            cosf, sinf = rope_of(b)
            kf = rope(kvp[:, :H], cosf, sinf)
            vf = kvp[:, H:]
            kv[blk(b), :] = kf.astype(BF16)
            vv[blk(b), :] = vf.astype(BF16)
            kT[:, blk(b)] = kf.T.astype(BF16)
            vT[:, blk(b)] = vf.T.astype(BF16)

        x_in(1).start()
        x_in(0).wait()
        normed(0)
        n_out(0).start()
        w_loads[0].wait()

        @pl.loop(0, NB - 1)
        def _(b):
            x_in(b + 1).wait()

            @pl.when(b + 2 < NB)
            def _():
                x_in(b + 2).start()

            @pl.when(b + 2 == NB)
            def _():
                y_in(0).start()

            @pl.when(b >= 1)
            def _():
                n_out(b - 1).wait()

            normed(b + 1)
            keys_values(b)
            n_out(b + 1).start()

        keys_values(NB - 1)
        n_out(NB - 2).wait()
        n_out(NB - 1).wait()

        def outs(t):
            s, i = lax.rem(t, 2), NB - 1 - t
            return [pltpu.make_async_copy(gst.at[s], g_hbm.at[blk(i)], out_sem.at[0, s]),
                    pltpu.make_async_copy(dast.at[s], da_hbm.at[blk(i)], out_sem.at[1, s]),
                    pltpu.make_async_copy(dqkvst.at[s], dqkv_hbm.at[blk(i)], out_sem.at[2, s]),
                    pltpu.make_async_copy(ost.at[s], o_hbm.at[blk(i)], out_sem.at[3, s])]

        for w in w_loads[1:]:
            w.wait()

        @pl.loop(0, NB)
        def _(t):
            slot = lax.rem(t, 2)
            i = NB - 1 - t
            yslot = lax.rem(t + 1, 2)

            @pl.when(t >= 2)
            def _():
                n_in(t).wait()
                for cp in outs(t - 2):
                    cp.wait()

            y_in(t).wait()

            @pl.when((t >= 1) & (t + 1 < NB))
            def _():
                n_in(t + 1).start()

            @pl.when(t + 1 < NB)
            def _():
                y_in(t + 1).start()

            points = service_points(plan[0], t)
            service(points[0])

            FT = min(512, F)
            for f in range(0, F, FT):
                a = mm(nbuf[slot], w1[:, f:f + FT])
                da = mm_nt(ybuf[yslot], w2[f:f + FT, :])
                phi = 0.5 + 0.5 * lax.erf(a * 0.7071067811865476)
                gst[slot, :, f:f + FT] = (a * phi).astype(BF16)
                dast[slot, :, f:f + FT] = (da * (phi + a * (0.3989422804014327 * jnp.exp(-0.5 * (a * a))))).astype(BF16)

            cosf, sinf = rope_of(i)
            qf = rope(mm(nbuf[slot], wqkv[:, :H]), cosf, sinf).astype(BF16).astype(F32) * (H ** -0.5)
            qs[...] = qf.astype(BF16)
            qT[...] = qf.T.astype(BF16)
            dof = mm_nt(ybuf[yslot], wo[...])
            do[...] = dof.astype(BF16)
            doT[...] = dof.T.astype(BF16)
            g_out, da_out, dqkv_out, o_out = outs(t)
            g_out.start()
            da_out.start()

            @pl.when(t > 0)
            def _():
                pair_sum(t - 1)

            service(points[1])

            nfull = i // QPC

            def chunk(j):
                return pl.ds(pl.multiple_of(j * C, C), C)

            def pass_a(j, carry, masked):
                m, l, dl = carry
                for u in range(QPC):
                    keys = pl.ds(pl.multiple_of(j * C + u * R, R), R)
                    st = mm(kv[keys, :], qT[...])
                    if masked:
                        key = j * C + u * R + lax.broadcasted_iota(jnp.int32, st.shape, 0)
                        query = i * R + lax.broadcasted_iota(jnp.int32, st.shape, 1)
                        st = jnp.where(key <= query, st, NEG)
                    dp = mm(vv[keys, :], doT[...])
                    m_new = jnp.maximum(m, jnp.max(st, axis=0, keepdims=True))
                    alpha = jnp.exp(m - m_new)
                    e = jnp.exp(st - m_new)
                    es[keys, :] = e
                    dps[keys, :] = dp
                    msc[pl.ds(j * QPC + u, 1), :] = m_new
                    m, l, dl = m_new, l * alpha + jnp.sum(e, axis=0, keepdims=True), dl * alpha + jnp.sum(e * dp, axis=0, keepdims=True)
                return m, l, dl

            init = (jnp.full((1, R), NEG, F32), jnp.zeros((1, R), F32), jnp.zeros((1, R), F32))
            carry = lax.fori_loop(0, nfull, functools.partial(pass_a, masked=False), init)
            m, l, dl = pass_a(nfull, carry, True)
            service(points[2])
            inv_l = 1.0 / l
            delta = dl * inv_l
            oT[...] = jnp.zeros_like(oT)
            dqT[...] = jnp.zeros_like(dqT)

            @pl.loop(0, nfull + 1)
            def _(j):
                pbs, dss = [], []
                for u in range(QPC):
                    keys = pl.ds(pl.multiple_of(j * C + u * R, R), R)
                    p = es[keys, :] * (jnp.exp(msc[pl.ds(j * QPC + u, 1), :] - m) * inv_l)
                    pbs.append(p.astype(BF16))
                    dss.append((p * (dps[keys, :] - delta)).astype(BF16))
                pb, ds = jnp.concatenate(pbs, axis=0), jnp.concatenate(dss, axis=0)
                oT[...] += mm(vT[:, chunk(j)], pb)
                dqT[...] += mm(kT[:, chunk(j)], ds)
                dv[chunk(j), :] += mm(pb, do[...])
                dk[chunk(j), :] += mm(ds, qs[...])

            service(points[3])

            EARLY = min(4 * R, T, D)
            for c in range(0, EARLY, R):
                es[c:c + R, :] = mm_nt(dast[slot], w1[c:c + R, :])

            ost[slot] = oT[...].T.astype(BF16)
            dqkvst[slot, :, :H] = rope(dqT[...].T * (H ** -0.5), cosf, -sinf).astype(BF16)
            dqkvst[slot, :, H:2 * H] = rope(dk[blk(i), :], cosf, -sinf).astype(BF16)
            dqkvst[slot, :, 2 * H:] = dv[blk(i), :].astype(BF16)
            dqkv_out.start()
            o_out.start()

            DT = min(512, D)
            for c in range(0, EARLY, R):
                pst[:, c:c + R] = (es[c:c + R, :] + mm_nt(dqkvst[slot], wqkv[c:c + R, :])).astype(BF16)
            for c in range(EARLY, D, DT):
                pst[:, c:c + DT] = (mm_nt(dast[slot], w1[c:c + DT, :]) + mm_nt(dqkvst[slot], wqkv[c:c + DT, :])).astype(BF16)
            sib_copy(t).start()

        for t in (NB - 2, NB - 1):
            for cp in outs(t):
                cp.wait()

    pl.run_scoped(
        attention_phase,
        pltpu.VMEM((T, H), BF16), pltpu.VMEM((H, T), BF16), pltpu.VMEM((T, H), BF16), pltpu.VMEM((H, T), BF16),
        pltpu.VMEM((T, H), F32), pltpu.VMEM((T, H), F32), pltpu.VMEM((T, R), F32), pltpu.VMEM((T, R), F32),
        pltpu.VMEM((D, F), BF16), pltpu.VMEM((F, D), BF16), pltpu.VMEM((D, 3 * H), BF16), pltpu.VMEM((H, D), BF16),
        pltpu.VMEM((2, R, D), BF16), pltpu.VMEM((2, R, D), BF16), pltpu.VMEM((2, R, F), BF16), pltpu.VMEM((2, R, F), BF16),
        pltpu.VMEM((2, R, 3 * H), BF16), pltpu.VMEM((2, R, H), BF16),
        pltpu.VMEM((R, H), BF16), pltpu.VMEM((H, R), BF16), pltpu.VMEM((R, H), BF16), pltpu.VMEM((H, R), BF16),
        pltpu.VMEM((H, R), F32), pltpu.VMEM((H, R), F32), pltpu.VMEM((max(8, NB), R), F32))

    NT1, NT2 = D // H, F // H

    def weight_phase(da, dqkv, dy, nt, w1st, wqst, w2st):
        loads = [pltpu.make_async_copy(s, d_, w_sem.at[k]) for k, (s, d_) in enumerate(((da_hbm, da), (dqkv_hbm, dqkv), (dy_hbm, dy)))]

        def cols(m):
            return pl.ds(pl.multiple_of(m * H, H), H)

        def nt_in(m):
            return pltpu.make_async_copy(n_hbm.at[:, cols(m)], nt.at[lax.rem(m, 2)], t2_sem.at[0, lax.rem(m, 2)])

        def g_in(m):
            return pltpu.make_async_copy(g_hbm.at[:, cols(m)], nt.at[lax.rem(m, 2)], t2_sem.at[0, lax.rem(m, 2)])

        def o_in():
            return pltpu.make_async_copy(o_hbm, nt.at[NT2 % 2], t2_sem.at[0, NT2 % 2])

        def out1(m):
            s = lax.rem(m, 2)
            return [pltpu.make_async_copy(w1st.at[s], dw1_hbm.at[cols(m)], t2_sem.at[1, s]),
                    pltpu.make_async_copy(wqst.at[s], dwqkv_hbm.at[cols(m)], t2_sem.at[2, s])]

        def out2(m):
            return pltpu.make_async_copy(w2st.at[lax.rem(m, 2)], dw2_hbm.at[cols(m)], t2_sem.at[1, lax.rem(m, 2)])

        def out3():
            return pltpu.make_async_copy(w2st.at[NT2 % 2], dwo_hbm, t2_sem.at[1, NT2 % 2])

        nt_in(0).start()
        loads[1].start()
        loads[0].start()
        loads[2].start()
        pair_sum(NB - 1)

        @pl.loop(0, NT1)
        def _(m):
            s = lax.rem(m, 2)
            nt_in(m).wait()

            @pl.when(m + 1 < NT1)
            def _():
                nt_in(m + 1).start()

            @pl.when(m + 1 == NT1)
            def _():
                g_in(0).start()

            @pl.when(m >= 2)
            def _():
                for cp in out1(m - 2):
                    cp.wait()

            points = service_points(plan[1], m)
            service(points[0])

            @pl.when(m == 0)
            def _():
                loads[1].wait()

            wqst[s] = mm_tn(nt[s], dqkv[...]).astype(BF16)
            service(points[1])

            @pl.when(m == 0)
            def _():
                loads[0].wait()

            w1st[s] = mm_tn(nt[s], da[...]).astype(BF16)
            for cp in out1(m):
                cp.start()

        for m in (NT1 - 2, NT1 - 1):
            for cp in out1(m):
                cp.wait()
        loads[2].wait()

        @pl.loop(0, NT2)
        def _(m):
            s = lax.rem(m, 2)
            g_in(m).wait()

            @pl.when(m + 1 < NT2)
            def _():
                g_in(m + 1).start()

            @pl.when(m + 1 == NT2)
            def _():
                o_in().start()

            @pl.when(m >= 2)
            def _():
                out2(m - 2).wait()

            points = service_points(plan[1], NT1 + m)
            service(points[0])
            w2st[s, :, :D // 2] = mm_tn(nt[s], dy[:, :D // 2]).astype(BF16)
            service(points[1])
            w2st[s, :, D // 2:] = mm_tn(nt[s], dy[:, D // 2:]).astype(BF16)
            out2(m).start()

        o_in().wait()
        out2(NT2 - 2).wait()
        points = service_points(plan[1], NT1 + NT2)
        service(points[0])
        w2st[NT2 % 2, :, :D // 2] = mm_tn(nt[NT2 % 2], dy[:, :D // 2]).astype(BF16)
        service(points[1])
        w2st[NT2 % 2, :, D // 2:] = mm_tn(nt[NT2 % 2], dy[:, D // 2:]).astype(BF16)
        out3().start()
        out2(NT2 - 1).wait()
        out3().wait()

    pl.run_scoped(
        weight_phase,
        pltpu.VMEM((T, F), BF16), pltpu.VMEM((T, 3 * H), BF16), pltpu.VMEM((T, D), BF16), pltpu.VMEM((2, T, H), BF16),
        pltpu.VMEM((2, H, F), BF16), pltpu.VMEM((2, H, 3 * H), BF16), pltpu.VMEM((2, H, D), BF16))

    (l3, l4, l5), last3, last4 = plan[2]
    service(([l3, l4, l5], [jnp.int32(last3), jnp.int32(last4)], [jnp.int32(0)] * 3))

    @pl.when(is_mid)
    def _():
        @pl.loop(0, NS - l4)
        def _(k):
            @pl.when(l3 + k < NS)
            def _():
                e3_fetch(l3 + k)
                e3_process(l3 + k)

            e4_fetch(l4 + k)
            e4_process(l4 + k)

        @pl.loop(0, NS)
        def _(t):
            dx_local(t).wait()
            dx_sib(t).wait_send()
            dx_out(t).wait_send()
            dx_sib(t).wait_recv()

    @pl.when(is_out)
    def _():
        @pl.loop(l5, NS)
        def _(t):
            e5(t)

        @pl.loop(0, NS)
        def _(t):
            q_copy(t).wait_send()
            dx_fwd(t).wait_send()
            dx_fwd(t).wait_recv()


def service_plan(blocks, tiles, keys_per_chunk):
    wire, lat, slow, count = 5.65, 2.5, 1.08, 2 * blocks
    at, ready, now = [], [], 14.0
    for t in range(blocks):
        chunks = (blocks - 1 - t) * ROWS // keys_per_chunk + 1
        mlp = now + 3.2 * slow
        at += [now, mlp, mlp + 0.56 * chunks * slow, mlp + 1.28 * chunks * slow]
        if t:
            ready += [mlp, mlp]
        now = at[-1] + 2.3 * slow
    ready += [now + 0.5, now + 0.5]
    now += 2.0
    for m in range(tiles):
        at += [now, now + 2.1 * slow]
        now += 4.3 * slow
    at.append(now)
    fires = []
    for step in range(3):
        table, sent, free, k = [], [], 0.0, 0
        for t in range(count):
            free = max(free, ready[t]) + wire
            while k < len(at) - 1 and at[k] < free + lat:
                k += 1
            if k < len(at) - 1:
                table.append(k)
                sent.append(at[k + 1])
                k += 1
            else:
                sent.append(free + lat)
        fires.append(set(table))
        ready = sent
    done, last, tables = [0, 0, 0], [0, 0], []
    k = 0
    for units, points in ((blocks, 4), (tiles, 2)):
        starts, codes = [], []
        for _ in range(units):
            starts.append(done[0] + 64 * done[1] + 4096 * done[2] + 262144 * last[0] + 524288 * last[1])
            code = 0
            for p in range(points):
                f = [int(k in fire) for fire in fires]
                code += sum(v * 2 ** (3 * p + step) for step, v in enumerate(f))
                done = [a + b for a, b in zip(done, f)]
                last = f[:2]
                k += 1
            codes.append(code)
        tables.append((tuple(starts), tuple(codes), points))
    return tables[0], tables[1], (tuple(done), last[0], last[1])


def copy_kernel(*refs):
    n = len(refs) // 4
    pieces = []
    for src, dst, buf, sem in zip(refs[:n], refs[n:2 * n], refs[2 * n:3 * n], refs[3 * n:]):
        count = sem.shape[1]
        rows = src.shape[0] // count
        for p in range(count):
            part = pl.ds(p * rows, rows)
            pieces.append((pltpu.make_async_copy(src.at[part], buf.at[part], sem.at[0, p]), pltpu.make_async_copy(buf.at[part], dst.at[part], sem.at[1, p])))
    for load, _ in pieces:
        load.start()
    for load, store in pieces:
        load.wait()
        store.start()
    for _, store in pieces:
        store.wait()


def copy_out(arrays):
    any_spec = pl.BlockSpec(memory_space=pl.ANY)
    counts = [2 ** max(0, (a.size // (512 * 1024)).bit_length() - 1) for a in arrays]
    size = sum(a.size * 2 for a in arrays)
    return pl.pallas_call(
        copy_kernel, name="results",
        out_shape=[jax.ShapeDtypeStruct(a.shape, a.dtype) for a in arrays],
        in_specs=[any_spec] * len(arrays), out_specs=[any_spec] * len(arrays),
        scratch_shapes=[pltpu.VMEM(a.shape, a.dtype) for a in arrays] + [pltpu.SemaphoreType.DMA((2, c)) for c in counts],
        compiler_params=pltpu.CompilerParams(vmem_limit_bytes=size + (4 << 20)))(*arrays)


def rope_tables(blocks, head_dim):
    rot = head_dim // 4
    half = rot // 2
    inv_freq = np.power(np.float32(10000.0), (-2.0 * np.arange(half, dtype=np.float32) / rot).astype(np.float32)).astype(np.float64)
    freq = np.zeros((1, 128))
    freq[0, :half], freq[0, half:rot] = -inv_freq, inv_freq
    at = np.arange(blocks)[:, None] * ROWS * freq
    off = np.arange(ROWS)[:, None] * freq
    return [np.asarray(t, np.float32) for t in (np.cos(at), np.sin(at), np.cos(off), np.sin(off))]


def solution(mesh):
    def device_step(resid_x, ln_mean, ln_rstd, ln_gain, grad_y, w_qkv, w_out, w_up, w_down):
        T, D = resid_x.shape
        F = w_up.shape[1]
        H = w_out.shape[1]
        NB = T // ROWS
        HALF = ROWS // 2
        C = min(1024, T)
        tabs = [jnp.asarray(t) for t in rope_tables(NB, H)]
        any_spec = pl.BlockSpec(memory_space=pl.ANY)
        vmem = pl.BlockSpec(memory_space=pltpu.VMEM)
        sds = lambda *s: jax.ShapeDtypeStruct(s, BF16)
        outs = pl.pallas_call(
            functools.partial(layer_kernel, (T, D, F, H, C), service_plan(NB, D // H + F // H + 1, C)),
            name="layer_backward",
            out_shape=[sds(T, D), sds(D, 3 * H), sds(H, D), sds(D, F), sds(F, D),
                       sds(T, D), sds(T, F), sds(T, F), sds(T, 3 * H), sds(T, H), sds(2 * NB, HALF // 2, D), sds(2 * NB, HALF // 2, D)],
            in_specs=[any_spec, any_spec] + [vmem] * 7 + [any_spec, any_spec, any_spec, any_spec],
            out_specs=[any_spec] * 12,
            scratch_shapes=[
                pltpu.VMEM((2 * NB, HALF // 2, D), BF16), pltpu.VMEM((ROWS, D), BF16), pltpu.VMEM((2, HALF, D), BF16),
                *[pltpu.VMEM((HALF // 2, D), BF16)] * 4,
                pltpu.SemaphoreType.DMA((2,)), pltpu.SemaphoreType.DMA((2,))]
            + [pltpu.SemaphoreType.DMA((2 * NB,))] * 8
            + [pltpu.SemaphoreType.DMA((4,)), pltpu.SemaphoreType.DMA((2, 2)), pltpu.SemaphoreType.DMA((4,)), pltpu.SemaphoreType.DMA((4, 2)),
               pltpu.SemaphoreType.DMA((3, 2))],
            compiler_params=pltpu.CompilerParams(collective_id=0, has_side_effects=True, vmem_limit_bytes=67043328),
        )(resid_x, grad_y, ln_gain.astype(F32).reshape(1, D), ln_mean.reshape(NB, ROWS), ln_rstd.reshape(NB, ROWS), *tabs, w_qkv, w_out.reshape(H, D), w_up, w_down)
        grad_x, grad_w_qkv, grad_w_out, grad_w_up, grad_w_down = copy_out(outs[:5])
        return grad_x, grad_w_qkv, grad_w_out.reshape(1, H, D), grad_w_up, grad_w_down

    in_specs = (P("data", None), P("data"), P("data"), P(None), P("data", None), P(None, "model"), P("model", None, None), P(None, "model"), P("model", None))
    out_specs = (P("data", None), P("data", "model"), P(("data", "model"), None, None), P("data", "model"), P(("data", "model"), None))
    return jax.shard_map(device_step, mesh=mesh, in_specs=in_specs, out_specs=out_specs, check_vma=False)
```

```python
import functools

import jax
import jax.numpy as jnp
import numpy as np
from jax import lax
from jax.experimental import pallas as pl
from jax.experimental.pallas import tpu as pltpu
from jax.sharding import PartitionSpec as P

MESH = pl.DeviceIdType.MESH
F32, BF16 = jnp.float32, jnp.bfloat16
ROWS = 256
NEG = -1e30


def mm(a, b):
    return jnp.dot(a, b, preferred_element_type=F32)


def mm_nt(a, b):
    return lax.dot_general(a, b, (((1,), (1,)), ((), ())), preferred_element_type=F32)


def mm_tn(a, b):
    return lax.dot_general(a, b, (((0,), (0,)), ((), ())), preferred_element_type=F32)


def clip(v, hi):
    return jnp.minimum(jnp.maximum(v, 0), hi)


def layer_kernel(dims, plan, x_hbm, dy_hbm, small_ref, cb_ref, sb_ref, co_ref, so_ref, wqkv_hbm, wo_hbm, w1_hbm, w2_hbm,
                 dx_hbm, dwqkv_hbm, dw1_hbm, n_hbm, g_hbm, da_hbm, dqkv_hbm, o_hbm, zin_hbm, xin_hbm,
                 gain, qbuf, pst, sib_in, zst, xst, lx, ly,
                 sib_s, sib_r, qs_s, z_r, x_r, dxl_s, dxs_s, dxo_s, dxo_r, dxs_r, st_sem, in_sem, w_sem, out_sem, t2_sem):
    T, D, F, H, C = dims
    R = ROWS
    HALF = R // 2
    PART = HALF // 2
    NB = T // R
    NS = 2 * NB
    QPC = C // R
    me = lax.axis_index("model")
    core = lax.rem(me, 2)
    z = me // 2
    nbz = z + 1 - 2 * lax.rem(z, 2)
    sibling = z * 2 + 1 - core
    near = nbz * 2 + core
    partner = (3 - z) * 2 + core
    is_mid = (z == 1) | (z == 2)
    is_out = (z == 0) | (z == 3)

    for c in range(D // R):
        gain[:, c * R:(c + 1) * R] = small_ref[2 * NB + c:2 * NB + c + 1, :]
    barrier = pltpu.get_barrier_semaphore()
    pl.semaphore_signal(barrier, inc=1, device_id={"model": sibling}, device_id_type=MESH)
    pl.semaphore_signal(barrier, inc=1, device_id={"model": near}, device_id_type=MESH)

    @pl.when(is_mid)
    def _():
        pl.semaphore_signal(barrier, inc=1, device_id={"model": partner}, device_id_type=MESH)
        pl.semaphore_wait(barrier, 3)

    @pl.when(is_out)
    def _():
        pl.semaphore_wait(barrier, 2)

    def rows_of(t, c):
        return pl.ds(pl.multiple_of((NB - 1 - t // 2) * R + c * HALF + lax.rem(t, 2) * PART, PART), PART)

    def sib_copy(t):
        s = lax.rem(t, 2)
        return pltpu.make_async_remote_copy(src_ref=pst.at[pl.ds(pl.multiple_of((1 - core) * HALF, HALF), HALF)], dst_ref=sib_in.at[s],
                                            send_sem=sib_s.at[s], recv_sem=sib_r.at[s], device_id={"model": sibling}, device_id_type=MESH)

    def q_copy(t):
        return pltpu.make_async_remote_copy(src_ref=qbuf.at[t], dst_ref=zin_hbm.at[t], send_sem=qs_s.at[t], recv_sem=z_r.at[t],
                                            device_id={"model": near}, device_id_type=MESH)

    def x_copy(t):
        return pltpu.make_async_remote_copy(src_ref=qbuf.at[t], dst_ref=xin_hbm.at[t], send_sem=qs_s.at[t], recv_sem=x_r.at[t],
                                            device_id={"model": partner}, device_id_type=MESH)

    def dx_local(t):
        return pltpu.make_async_copy(qbuf.at[t], dx_hbm.at[rows_of(t, core)], dxl_s.at[t])

    def dx_sib(t):
        return pltpu.make_async_remote_copy(src_ref=qbuf.at[t], dst_ref=dx_hbm.at[rows_of(t, core)], send_sem=dxs_s.at[t], recv_sem=dxs_r.at[t],
                                            device_id={"model": sibling}, device_id_type=MESH)

    def dx_out(t):
        return pltpu.make_async_remote_copy(src_ref=qbuf.at[t], dst_ref=dx_hbm.at[rows_of(t, core)], send_sem=dxo_s.at[t], recv_sem=dxo_r.at[t],
                                            device_id={"model": near}, device_id_type=MESH)

    def dx_fwd(t):
        return pltpu.make_async_remote_copy(src_ref=dx_hbm.at[rows_of(t, core)], dst_ref=dx_hbm.at[rows_of(t, core)], send_sem=dxs_s.at[t],
                                            recv_sem=dxs_r.at[t], device_id={"model": sibling}, device_id_type=MESH)

    def z_load(t):
        return pltpu.make_async_copy(zin_hbm.at[t], zst, st_sem.at[0])

    def x_load(t):
        return pltpu.make_async_copy(xin_hbm.at[t], xst, st_sem.at[1])

    def lx_load(t):
        return pltpu.make_async_copy(x_hbm.at[rows_of(t, core)], lx, st_sem.at[2])

    def ly_load(t):
        return pltpu.make_async_copy(dy_hbm.at[rows_of(t, core)], ly, st_sem.at[3])

    def pair_sum(t):
        cp = sib_copy(t)
        cp.wait_send()
        cp.wait_recv()
        for h in range(2):
            own = pst[pl.ds(pl.multiple_of(core * HALF + h * PART, PART), PART), :].astype(F32)
            qbuf[2 * t + h] = (own + sib_in[lax.rem(t, 2), h * PART:(h + 1) * PART, :].astype(F32)).astype(BF16)

            @pl.when(is_out)
            def _(h=h):
                q_copy(2 * t + h).start()

    def e3_fetch(t):
        q_copy(t).wait_recv()
        z_load(t).start()

    def e3_process(t):
        z_load(t).wait()
        qbuf[t] = (qbuf[t].astype(F32) + zst[...].astype(F32)).astype(BF16)
        x_copy(t).start()

    def e4_fetch(t):
        x_copy(t).wait_recv()
        x_load(t).start()
        lx_load(t).start()
        ly_load(t).start()

    def e4_process(t):
        x_load(t).wait()
        lx_load(t).wait()
        ly_load(t).wait()
        x_copy(t).wait_send()
        mean, rstd = row_stats(NB - 1 - t // 2, core * 2 + lax.rem(t, 2))
        xh = (lx[...].astype(F32) - mean) * rstd
        d = (qbuf[t].astype(F32) + xst[...].astype(F32)) * gain[...]
        md = jnp.sum(d, axis=1, keepdims=True) * (1.0 / D)
        mdx = jnp.sum(d * xh, axis=1, keepdims=True) * (1.0 / D)
        qbuf[t] = (ly[...].astype(F32) + rstd * (d - md - xh * mdx)).astype(BF16)
        dx_out(t).start()
        dx_sib(t).start()
        dx_local(t).start()

    def e5(t):
        dx_out(t).wait_recv()
        dx_fwd(t).start()

    def lookup(table, k):
        v = jnp.int32(table[0])
        for at in range(1, len(table)):
            v = jnp.where(k == at, table[at], v)
        return v

    def service_points(table, k):
        start, fire = lookup(table[0], k), lookup(table[1], k)
        c = [start % 64, (start // 64) % 64, (start // 4096) % 64]
        pend = [(start // 262144) % 2, (start // 524288) % 2]
        points = []
        for p in range(table[2]):
            f = [(fire // 2 ** (3 * p + step)) % 2 for step in range(3)]
            points.append((list(c), list(pend), f))
            c = [a + b for a, b in zip(c, f)]
            pend = f[:2]
        return points

    def service(point):
        c, pend, f = point

        @pl.when(is_mid & (pend[0] > 0))
        def _():
            e3_process(c[0] - 1)

        @pl.when(is_mid & (f[0] > 0))
        def _():
            e3_fetch(c[0])

        @pl.when(is_mid & (pend[1] > 0))
        def _():
            e4_process(c[1] - 1)

        @pl.when(is_mid & (f[1] > 0))
        def _():
            e4_fetch(c[1])

        @pl.when(is_out & (f[2] > 0))
        def _():
            e5(c[2])

    def row_stats(i, part=None):
        out = []
        for first in (0, NB):
            row = small_ref[pl.ds(first + i, 1), :]
            if part is None:
                col = jnp.broadcast_to(row, (128, R)).T
            else:
                row = jnp.where(part >= 2, row[:, HALF:], row[:, :HALF])
                col = jnp.broadcast_to(row, (128, HALF)).T
                col = jnp.where(lax.rem(part, 2) == 0, col[:PART], col[PART:])
            out.append(jnp.concatenate([col] * (D // 128), axis=1))
        return out

    def rope_of(i):
        cb, sb = cb_ref[pl.ds(i, 1), :], sb_ref[pl.ds(i, 1), :]
        co, so = co_ref[...], so_ref[...]
        return cb * co - sb * so, sb * co + cb * so

    def rope(x, cosf, sinf):
        x0 = x[:, :128]
        lane = lax.broadcasted_iota(jnp.int32, x0.shape, 1)
        other = jnp.where(lane < H // 8, pltpu.roll(x0, 128 - H // 8, 1), pltpu.roll(x0, H // 8, 1))
        return jnp.concatenate([x0 * cosf + other * sinf, x[:, 128:]], axis=1)

    def attention_phase(kv, kT, vv, vT, dk, dv, es, dps, w1, w2, wqkv, wo, nbuf, ybuf, gst, dast, dqkvst, ost, qs, qT, do, doT, oT, dqT, msc, stat):
        w_loads = [pltpu.make_async_copy(s, d_, w_sem.at[k]) for k, (s, d_) in enumerate(((wqkv_hbm, wqkv), (wo_hbm, wo), (w1_hbm, w1), (w2_hbm, w2)))]

        def blk(i):
            return pl.ds(pl.multiple_of(i * R, R), R)

        def x_in(b):
            return pltpu.make_async_copy(x_hbm.at[blk(b)], ybuf.at[lax.rem(b + 1, 2)], in_sem.at[0, lax.rem(b + 1, 2)])

        def n_out(b):
            return pltpu.make_async_copy(nbuf.at[lax.rem(b + 1, 2)], n_hbm.at[blk(b)], out_sem.at[0, lax.rem(b + 1, 2)])

        def n_in(t):
            return pltpu.make_async_copy(n_hbm.at[blk(NB - 1 - t)], nbuf.at[lax.rem(t, 2)], in_sem.at[1, lax.rem(t, 2)])

        def y_in(t):
            return pltpu.make_async_copy(dy_hbm.at[blk(NB - 1 - t)], ybuf.at[lax.rem(t + 1, 2)], in_sem.at[0, lax.rem(t + 1, 2)])

        w_loads[0].start()
        x_in(0).start()
        for w in w_loads[1:]:
            w.start()
        dk[...] = jnp.zeros_like(dk)
        dv[...] = jnp.zeros_like(dv)

        def normed(b):
            slot = lax.rem(b + 1, 2)
            mean, rstd = row_stats(b)
            nbuf[slot] = (((ybuf[slot].astype(F32) - mean) * rstd) * gain[...]).astype(BF16)

        def keys_values(b):
            kvp = mm(nbuf[lax.rem(b + 1, 2)], wqkv[:, H:])
            cosf, sinf = rope_of(b)
            kf = rope(kvp[:, :H], cosf, sinf)
            vf = kvp[:, H:]
            kv[blk(b), :] = kf.astype(BF16)
            vv[blk(b), :] = vf.astype(BF16)
            kT[:, blk(b)] = kf.T.astype(BF16)
            vT[:, blk(b)] = vf.T.astype(BF16)

        x_in(1).start()
        x_in(0).wait()
        normed(0)
        n_out(0).start()
        w_loads[0].wait()

        @pl.loop(0, NB - 1)
        def _(b):
            x_in(b + 1).wait()

            @pl.when(b + 2 < NB)
            def _():
                x_in(b + 2).start()

            @pl.when(b + 2 == NB)
            def _():
                y_in(0).start()

            @pl.when(b >= 1)
            def _():
                n_out(b - 1).wait()

            normed(b + 1)
            keys_values(b)
            n_out(b + 1).start()

        keys_values(NB - 1)
        n_out(NB - 2).wait()
        n_out(NB - 1).wait()

        def outs(t):
            s, i = lax.rem(t, 2), NB - 1 - t
            return [pltpu.make_async_copy(gst.at[s], g_hbm.at[blk(i)], out_sem.at[0, s]),
                    pltpu.make_async_copy(dast.at[s], da_hbm.at[blk(i)], out_sem.at[1, s]),
                    pltpu.make_async_copy(dqkvst.at[s], dqkv_hbm.at[blk(i)], out_sem.at[2, s]),
                    pltpu.make_async_copy(ost.at[s], o_hbm.at[blk(i)], out_sem.at[3, s])]

        for w in w_loads[1:]:
            w.wait()

        @pl.loop(0, NB)
        def _(t):
            slot = lax.rem(t, 2)
            i = NB - 1 - t
            yslot = lax.rem(t + 1, 2)

            @pl.when(t >= 2)
            def _():
                n_in(t).wait()
                for cp in outs(t - 2):
                    cp.wait()

            y_in(t).wait()

            @pl.when((t >= 1) & (t + 1 < NB))
            def _():
                n_in(t + 1).start()

            @pl.when(t + 1 < NB)
            def _():
                y_in(t + 1).start()

            points = service_points(plan[0], t)
            service(points[0])

            FT = min(512, F)
            for f in range(0, F, FT):
                a = mm(nbuf[slot], w1[:, f:f + FT])
                da = mm_nt(ybuf[yslot], w2[f:f + FT, :])
                phi = 0.5 + 0.5 * lax.erf(a * 0.7071067811865476)
                gst[slot, :, f:f + FT] = (a * phi).astype(BF16)
                dast[slot, :, f:f + FT] = (da * (phi + a * (0.3989422804014327 * jnp.exp(-0.5 * (a * a))))).astype(BF16)

            cosf, sinf = rope_of(i)
            qf = rope(mm(nbuf[slot], wqkv[:, :H]), cosf, sinf).astype(BF16).astype(F32) * (H ** -0.5)
            qs[...] = qf.astype(BF16)
            qT[...] = qf.T.astype(BF16)
            dof = mm_nt(ybuf[yslot], wo[...])
            do[...] = dof.astype(BF16)
            doT[...] = dof.T.astype(BF16)
            g_out, da_out, dqkv_out, o_out = outs(t)
            g_out.start()
            da_out.start()

            @pl.when(t > 0)
            def _():
                pair_sum(t - 1)

            service(points[1])

            nfull = i // QPC

            below = jnp.where(lax.broadcasted_iota(jnp.int32, (R, R), 0) <= lax.broadcasted_iota(jnp.int32, (R, R), 1), 0.0, NEG)

            def part(j, u, n=1):
                return pl.ds(pl.multiple_of(j * C + u * R, R), n * R)

            def pass_a(j, carry, subs, diagonal):
                m, l, dl = carry
                for u in range(subs):
                    st = mm(kv[part(j, u), :], qT[...])
                    if diagonal and u == subs - 1:
                        st = jnp.where(below == 0.0, st, NEG)
                    dp = mm(vv[part(j, u), :], doT[...])
                    m_new = jnp.maximum(m, jnp.max(st, axis=0, keepdims=True))
                    alpha = jnp.exp(m - m_new)
                    e = jnp.exp(st - m_new)
                    es[part(j, u), :] = e
                    dps[part(j, u), :] = dp
                    msc[pl.ds(j * QPC + u, 1), :] = m_new
                    m, l, dl = m_new, l * alpha + jnp.sum(e, axis=0, keepdims=True), dl * alpha + jnp.sum(e * dp, axis=0, keepdims=True)
                return m, l, dl

            init = (jnp.full((1, R), NEG, F32), jnp.zeros((1, R), F32), jnp.zeros((1, R), F32))
            carry = lax.fori_loop(0, nfull, functools.partial(pass_a, subs=QPC, diagonal=False), init)
            for row, value in enumerate(carry):
                stat[row:row + 1, :] = value
            for v in range(QPC):
                @pl.when(lax.rem(i, QPC) == v)
                def _(v=v):
                    carry = pass_a(nfull, tuple(stat[row:row + 1, :] for row in range(3)), v + 1, True)
                    for row, value in enumerate(carry):
                        stat[row:row + 1, :] = value

            service(points[2])
            m = stat[0:1, :]
            inv_l = 1.0 / stat[1:2, :]
            delta = stat[2:3, :] * inv_l
            oT[...] = jnp.zeros_like(oT)
            dqT[...] = jnp.zeros_like(dqT)

            def pass_b(j, subs):
                pbs, dss = [], []
                for u in range(subs):
                    p = es[part(j, u), :] * (jnp.exp(msc[pl.ds(j * QPC + u, 1), :] - m) * inv_l)
                    pbs.append(p.astype(BF16))
                    dss.append((p * (dps[part(j, u), :] - delta)).astype(BF16))
                pb, ds = jnp.concatenate(pbs, axis=0), jnp.concatenate(dss, axis=0)
                keys = part(j, 0, subs)
                oT[...] += mm(vT[:, keys], pb)
                dqT[...] += mm(kT[:, keys], ds)
                dv[keys, :] += mm(pb, do[...])
                dk[keys, :] += mm(ds, qs[...])

            @pl.loop(0, nfull)
            def _(j):
                pass_b(j, QPC)

            for v in range(QPC):
                @pl.when(lax.rem(i, QPC) == v)
                def _(v=v):
                    pass_b(nfull, v + 1)

            service(points[3])

            EARLY = min(4 * R, T, D)
            for c in range(0, EARLY, R):
                es[c:c + R, :] = mm_nt(dast[slot], w1[c:c + R, :])

            ost[slot] = oT[...].T.astype(BF16)
            dqkvst[slot, :, :H] = rope(dqT[...].T * (H ** -0.5), cosf, -sinf).astype(BF16)
            dqkvst[slot, :, H:2 * H] = rope(dk[blk(i), :], cosf, -sinf).astype(BF16)
            dqkvst[slot, :, 2 * H:] = dv[blk(i), :].astype(BF16)
            dqkv_out.start()
            o_out.start()

            DT = min(512, D)
            for c in range(0, EARLY, R):
                pst[:, c:c + R] = (es[c:c + R, :] + mm_nt(dqkvst[slot], wqkv[c:c + R, :])).astype(BF16)
            for c in range(EARLY, D, DT):
                pst[:, c:c + DT] = (mm_nt(dast[slot], w1[c:c + DT, :]) + mm_nt(dqkvst[slot], wqkv[c:c + DT, :])).astype(BF16)
            sib_copy(t).start()

        for t in (NB - 2, NB - 1):
            for cp in outs(t):
                cp.wait()

    pl.run_scoped(
        attention_phase,
        pltpu.VMEM((T, H), BF16), pltpu.VMEM((H, T), BF16), pltpu.VMEM((T, H), BF16), pltpu.VMEM((H, T), BF16),
        pltpu.VMEM((T, H), F32), pltpu.VMEM((T, H), F32), pltpu.VMEM((T, R), F32), pltpu.VMEM((T, R), F32),
        pltpu.VMEM((D, F), BF16), pltpu.VMEM((F, D), BF16), pltpu.VMEM((D, 3 * H), BF16), pltpu.VMEM((H, D), BF16),
        pltpu.VMEM((2, R, D), BF16), pltpu.VMEM((2, R, D), BF16), pltpu.VMEM((2, R, F), BF16), pltpu.VMEM((2, R, F), BF16),
        pltpu.VMEM((2, R, 3 * H), BF16), pltpu.VMEM((2, R, H), BF16),
        pltpu.VMEM((R, H), BF16), pltpu.VMEM((H, R), BF16), pltpu.VMEM((R, H), BF16), pltpu.VMEM((H, R), BF16),
        pltpu.VMEM((H, R), F32), pltpu.VMEM((H, R), F32), pltpu.VMEM((max(8, NB), R), F32), pltpu.VMEM((8, R), F32))

    NT1 = D // H

    def weight_phase(da, dqkv, nt, w1st, wqst):
        loads = [pltpu.make_async_copy(s, d_, w_sem.at[k]) for k, (s, d_) in enumerate(((da_hbm, da), (dqkv_hbm, dqkv)))]

        def cols(m):
            return pl.ds(pl.multiple_of(m * H, H), H)

        def nt_in(m):
            return pltpu.make_async_copy(n_hbm.at[:, cols(m)], nt.at[lax.rem(m, 2)], t2_sem.at[0, lax.rem(m, 2)])

        def out1(m):
            s = lax.rem(m, 2)
            return [pltpu.make_async_copy(w1st.at[s], dw1_hbm.at[cols(m)], t2_sem.at[1, s]),
                    pltpu.make_async_copy(wqst.at[s], dwqkv_hbm.at[cols(m)], t2_sem.at[2, s])]

        nt_in(0).start()
        loads[1].start()
        loads[0].start()
        pair_sum(NB - 1)

        @pl.loop(0, NT1)
        def _(m):
            s = lax.rem(m, 2)
            nt_in(m).wait()

            @pl.when(m + 1 < NT1)
            def _():
                nt_in(m + 1).start()

            @pl.when(m >= 2)
            def _():
                for cp in out1(m - 2):
                    cp.wait()

            points = service_points(plan[1], m)
            service(points[0])

            @pl.when(m == 0)
            def _():
                loads[1].wait()

            wqst[s] = mm_tn(nt[s], dqkv[...]).astype(BF16)
            service(points[1])

            @pl.when(m == 0)
            def _():
                loads[0].wait()

            w1st[s] = mm_tn(nt[s], da[...]).astype(BF16)
            for cp in out1(m):
                cp.start()

        for m in (NT1 - 2, NT1 - 1):
            for cp in out1(m):
                cp.wait()

    pl.run_scoped(
        weight_phase,
        pltpu.VMEM((T, F), BF16), pltpu.VMEM((T, 3 * H), BF16), pltpu.VMEM((2, T, H), BF16),
        pltpu.VMEM((2, H, F), BF16), pltpu.VMEM((2, H, 3 * H), BF16))

    (l3, l4, l5), last3, last4 = plan[2]
    service(([l3, l4, l5], [jnp.int32(last3), jnp.int32(last4)], [jnp.int32(0)] * 3))

    @pl.when(is_mid)
    def _():
        @pl.loop(0, NS - l4)
        def _(k):
            @pl.when(l3 + k < NS)
            def _():
                e3_fetch(l3 + k)
                e3_process(l3 + k)

            e4_fetch(l4 + k)
            e4_process(l4 + k)

        @pl.loop(0, NS)
        def _(t):
            dx_local(t).wait()
            dx_sib(t).wait_send()
            dx_out(t).wait_send()
            dx_sib(t).wait_recv()

    @pl.when(is_out)
    def _():
        @pl.loop(l5, NS)
        def _(t):
            e5(t)

        @pl.loop(0, NS)
        def _(t):
            q_copy(t).wait_send()
            dx_fwd(t).wait_send()
            dx_fwd(t).wait_recv()


def service_plan(blocks, tiles):
    wire, lat, slow, count = 5.65, 2.5, 1.08, 2 * blocks
    at, ready, now = [], [], 20.5
    for t in range(blocks):
        keys = blocks - t
        mlp = now + 3.6
        at += [now, mlp, mlp + 0.4 + 0.14 * keys * slow, mlp + 0.8 + 0.32 * keys * slow]
        if t:
            ready += [mlp, mlp]
        now = at[-1] + 3.0
    ready += [now + 0.5, now + 0.5]
    now += 4.0
    for m in range(tiles):
        at += [now, now + 2.3]
        now += 5.0
    at.append(now)
    fires = []
    for step in range(3):
        table, sent, free, k = [], [], 0.0, 0
        for t in range(count):
            free = max(free, ready[t]) + wire
            while k < len(at) - 1 and at[k] < free + lat:
                k += 1
            if k < len(at) - 1:
                table.append(k)
                sent.append(at[k + 1])
                k += 1
            else:
                sent.append(free + lat)
        fires.append(set(table))
        ready = sent
    done, last, tables = [0, 0, 0], [0, 0], []
    k = 0
    for units, points in ((blocks, 4), (tiles, 2)):
        starts, codes = [], []
        for _ in range(units):
            starts.append(done[0] + 64 * done[1] + 4096 * done[2] + 262144 * last[0] + 524288 * last[1])
            code = 0
            for p in range(points):
                f = [int(k in fire) for fire in fires]
                code += sum(v * 2 ** (3 * p + step) for step, v in enumerate(f))
                done = [a + b for a, b in zip(done, f)]
                last = f[:2]
                k += 1
            codes.append(code)
        tables.append((tuple(starts), tuple(codes), points))
    return tables[0], tables[1], (tuple(done), last[0], last[1])


def finish_kernel(dims, dx_in, dwq_in, dw1_in, g_hbm, o_hbm, dy_hbm, dx_hbm, dwq_hbm, dw1_hbm, dw2_hbm, dwo_hbm,
                  go, dy, wst, xbuf, wqbuf, w1buf, g_sem, y_sem, out_sem, x_sem, q_sem, u_sem):
    T, D, F, H = dims
    M, W = F // H + 1, min(512, D)
    N = D // W
    XP = 16
    XR, UR = T // XP, D // 4

    def cols(k, w):
        return pl.ds(pl.multiple_of(k * w, w), w)

    def g_in(m):
        return pltpu.make_async_copy(g_hbm.at[:, cols(m, H)], go.at[m], g_sem.at[m])

    o_in = pltpu.make_async_copy(o_hbm, go.at[M - 1], g_sem.at[M - 1])

    def y_in(n):
        return pltpu.make_async_copy(dy_hbm.at[:, cols(n, W)], dy.at[n], y_sem.at[n])

    def x_copy(p):
        return (pltpu.make_async_copy(dx_in.at[cols(p, XR)], xbuf.at[cols(p, XR)], x_sem.at[0, p]),
                pltpu.make_async_copy(xbuf.at[cols(p, XR)], dx_hbm.at[cols(p, XR)], x_sem.at[1, p]))

    def u_copy(p):
        return (pltpu.make_async_copy(dw1_in.at[cols(p, UR)], w1buf.at[cols(p, UR)], u_sem.at[0, p]),
                pltpu.make_async_copy(w1buf.at[cols(p, UR)], dw1_hbm.at[cols(p, UR)], u_sem.at[1, p]))

    q_load = pltpu.make_async_copy(dwq_in, wqbuf, q_sem.at[0])
    q_store = pltpu.make_async_copy(wqbuf, dwq_hbm, q_sem.at[1])

    g_in(0).start()
    y_in(0).start()
    for m in range(1, M - 1):
        g_in(m).start()
    o_in.start()
    y_in(1).start() if N > 1 else None
    for p in range(4):
        x_copy(p)[0].start()

    def w2_out(k, m, n):
        return pltpu.make_async_copy(wst.at[lax.rem(k, 2)], dw2_hbm.at[cols(m, H), cols(n, W)], out_sem.at[lax.rem(k, 2)])

    def wo_out(k, n):
        return pltpu.make_async_copy(wst.at[lax.rem(k, 2)], dwo_hbm.at[:, cols(n, W)], out_sem.at[lax.rem(k, 2)])

    @pl.loop(0, N * M)
    def _(k):
        n, m = k // M, lax.rem(k, M)

        @pl.when(n == 0)
        def _():
            pltpu.make_async_copy(o_hbm, go.at[m], g_sem.at[m]).wait()

        @pl.when(m == 0)
        def _():
            y_in(n).wait()

            @pl.when(n + 2 < N)
            def _():
                y_in(n + 2).start()

        @pl.when(k + 4 < XP)
        def _():
            x_copy(k + 4)[0].start()

        @pl.when((k + 4 >= XP) & (k + 4 < XP + 4))
        def _():
            u_copy(k + 4 - XP)[0].start()

        @pl.when(k == 2)
        def _():
            q_load.start()

        @pl.when(k == 6)
        def _():
            q_load.wait()
            q_store.start()

        @pl.when(k >= 2)
        def _():
            wo_out(k, 0).wait()

        wst[lax.rem(k, 2)] = mm_tn(go[m], dy[n]).astype(BF16)

        @pl.when(m < M - 1)
        def _():
            w2_out(k, m, n).start()

        @pl.when(m == M - 1)
        def _():
            wo_out(k, n).start()

        @pl.when(k < XP)
        def _():
            load, store = x_copy(k)
            load.wait()
            store.start()

        @pl.when((k >= XP) & (k < XP + 4))
        def _():
            load, store = u_copy(k - XP)
            load.wait()
            store.start()

    for k in range(N * M, XP + 4):
        load, store = x_copy(k) if k < XP else u_copy(k - XP)
        if k >= N * M + 4:
            load.start()
        load.wait()
        store.start()
    for k in (N * M - 2, N * M - 1):
        wo_out(k, 0).wait()
    q_store.wait()
    for p in range(XP):
        x_copy(p)[1].wait()
    for p in range(4):
        u_copy(p)[1].wait()


def finish(dx, dwq, dw1, act, attn, dy):
    (T, D), F, H = dx.shape, act.shape[1], attn.shape[1]
    W = min(512, D)
    any_spec = pl.BlockSpec(memory_space=pl.ANY)
    return pl.pallas_call(
        functools.partial(finish_kernel, (T, D, F, H)), name="finish",
        out_shape=[jax.ShapeDtypeStruct(sh, BF16) for sh in (dx.shape, dwq.shape, dw1.shape, (F, D), (H, D))],
        in_specs=[any_spec] * 6, out_specs=[any_spec] * 5,
        scratch_shapes=[pltpu.VMEM((F // H + 1, T, H), BF16), pltpu.VMEM((D // W, T, W), BF16), pltpu.VMEM((2, H, W), BF16),
                        pltpu.VMEM(dx.shape, BF16), pltpu.VMEM(dwq.shape, BF16), pltpu.VMEM(dw1.shape, BF16),
                        pltpu.SemaphoreType.DMA((F // H + 1,)), pltpu.SemaphoreType.DMA((D // W,)), pltpu.SemaphoreType.DMA((2,)),
                        pltpu.SemaphoreType.DMA((2, 16)), pltpu.SemaphoreType.DMA((2,)), pltpu.SemaphoreType.DMA((2, 4))],
        compiler_params=pltpu.CompilerParams(vmem_limit_bytes=67043328))(dx, dwq, dw1, act, attn, dy)


def rope_tables(blocks, head_dim):
    rot = head_dim // 4
    half = rot // 2
    inv_freq = np.power(np.float32(10000.0), (-2.0 * np.arange(half, dtype=np.float32) / rot).astype(np.float32)).astype(np.float64)
    freq = np.zeros((1, 128))
    freq[0, :half], freq[0, half:rot] = -inv_freq, inv_freq
    at = np.arange(blocks)[:, None] * ROWS * freq
    off = np.arange(ROWS)[:, None] * freq
    return [np.asarray(t, np.float32) for t in (np.cos(at), np.sin(at), np.cos(off), np.sin(off))]


def solution(mesh):
    def device_step(resid_x, ln_mean, ln_rstd, ln_gain, grad_y, w_qkv, w_out, w_up, w_down):
        T, D = resid_x.shape
        F = w_up.shape[1]
        H = w_out.shape[1]
        NB = T // ROWS
        HALF = ROWS // 2
        C = min(1024, T)
        tabs = [jnp.asarray(t) for t in rope_tables(NB, H)]
        small = jnp.concatenate([ln_mean, ln_rstd, ln_gain.astype(F32)]).reshape(2 * NB + D // ROWS, ROWS)
        any_spec = pl.BlockSpec(memory_space=pl.ANY)
        vmem = pl.BlockSpec(memory_space=pltpu.VMEM)
        sds = lambda *s: jax.ShapeDtypeStruct(s, BF16)
        outs = pl.pallas_call(
            functools.partial(layer_kernel, (T, D, F, H, C), service_plan(NB, D // H)),
            name="layer_backward",
            out_shape=[sds(T, D), sds(D, 3 * H), sds(D, F),
                       sds(T, D), sds(T, F), sds(T, F), sds(T, 3 * H), sds(T, H), sds(2 * NB, HALF // 2, D), sds(2 * NB, HALF // 2, D)],
            in_specs=[any_spec, any_spec] + [vmem] * 5 + [any_spec, any_spec, any_spec, any_spec],
            out_specs=[any_spec] * 10,
            scratch_shapes=[
                pltpu.VMEM((1, D), F32), pltpu.VMEM((2 * NB, HALF // 2, D), BF16), pltpu.VMEM((ROWS, D), BF16), pltpu.VMEM((2, HALF, D), BF16),
                *[pltpu.VMEM((HALF // 2, D), BF16)] * 4,
                pltpu.SemaphoreType.DMA((2,)), pltpu.SemaphoreType.DMA((2,))]
            + [pltpu.SemaphoreType.DMA((2 * NB,))] * 8
            + [pltpu.SemaphoreType.DMA((4,)), pltpu.SemaphoreType.DMA((2, 2)), pltpu.SemaphoreType.DMA((4,)), pltpu.SemaphoreType.DMA((4, 2)),
               pltpu.SemaphoreType.DMA((3, 2))],
            compiler_params=pltpu.CompilerParams(collective_id=0, has_side_effects=True, vmem_limit_bytes=67043328),
        )(resid_x, grad_y, small, *tabs, w_qkv, w_out.reshape(H, D), w_up, w_down)
        grad_x, grad_w_qkv, grad_w_up, _, act, _, _, attn, _, _ = outs
        grad_x, grad_w_qkv, grad_w_up, grad_w_down, grad_w_out = finish(grad_x, grad_w_qkv, grad_w_up, act, attn, grad_y)
        return grad_x, grad_w_qkv, grad_w_out.reshape(1, H, D), grad_w_up, grad_w_down

    in_specs = (P("data", None), P("data"), P("data"), P(None), P("data", None), P(None, "model"), P("model", None, None), P(None, "model"), P("model", None))
    out_specs = (P("data", None), P("data", "model"), P(("data", "model"), None, None), P("data", "model"), P(("data", "model"), None))
    return jax.shard_map(device_step, mesh=mesh, in_specs=in_specs, out_specs=out_specs, check_vma=False)
```

```python
import functools

import jax
import jax.numpy as jnp
import numpy as np
from jax import lax
from jax.experimental import pallas as pl
from jax.experimental.pallas import tpu as pltpu
from jax.sharding import PartitionSpec as P

MESH = pl.DeviceIdType.MESH
F32, BF16 = jnp.float32, jnp.bfloat16
ROWS = 256
NEG = -1e30


def mm(a, b):
    return jnp.dot(a, b, preferred_element_type=F32)


def mm_nt(a, b):
    return lax.dot_general(a, b, (((1,), (1,)), ((), ())), preferred_element_type=F32)


def mm_tn(a, b):
    return lax.dot_general(a, b, (((0,), (0,)), ((), ())), preferred_element_type=F32)


def clip(v, hi):
    return jnp.minimum(jnp.maximum(v, 0), hi)


def layer_kernel(dims, plan, x_hbm, dy_hbm, small_ref, cb_ref, sb_ref, co_ref, so_ref, wqkv_hbm, wo_hbm, w1_hbm, w2_hbm,
                 dx_hbm, dwqkv_hbm, dwo_hbm, dw1_hbm, dw2_hbm, n_hbm, g_hbm, da_hbm, dqkv_hbm, o_hbm, zin_hbm, xin_hbm,
                 gain, qbuf, pst, sib_in, zst, xst, lx, ly,
                 sib_s, sib_r, qs_s, z_r, x_r, dxl_s, dxs_s, dxo_s, dxo_r, dxs_r, st_sem, in_sem, w_sem, out_sem, t2_sem):
    T, D, F, H, C = dims
    R = ROWS
    HALF = R // 2
    PART = HALF // 2
    NB = T // R
    NS = 2 * NB
    QPC = C // R
    me = lax.axis_index("model")
    core = lax.rem(me, 2)
    z = me // 2
    nbz = z + 1 - 2 * lax.rem(z, 2)
    sibling = z * 2 + 1 - core
    near = nbz * 2 + core
    partner = (3 - z) * 2 + core
    is_mid = (z == 1) | (z == 2)
    is_out = (z == 0) | (z == 3)

    for c in range(D // R):
        gain[:, c * R:(c + 1) * R] = small_ref[2 * NB + c:2 * NB + c + 1, :]
    barrier = pltpu.get_barrier_semaphore()
    pl.semaphore_signal(barrier, inc=1, device_id={"model": sibling}, device_id_type=MESH)
    pl.semaphore_signal(barrier, inc=1, device_id={"model": near}, device_id_type=MESH)

    @pl.when(is_mid)
    def _():
        pl.semaphore_signal(barrier, inc=1, device_id={"model": partner}, device_id_type=MESH)
        pl.semaphore_wait(barrier, 3)

    @pl.when(is_out)
    def _():
        pl.semaphore_wait(barrier, 2)

    def rows_of(t, c):
        return pl.ds(pl.multiple_of((NB - 1 - t // 2) * R + c * HALF + lax.rem(t, 2) * PART, PART), PART)

    def sib_copy(t):
        s = lax.rem(t, 2)
        return pltpu.make_async_remote_copy(src_ref=pst.at[pl.ds(pl.multiple_of((1 - core) * HALF, HALF), HALF)], dst_ref=sib_in.at[s],
                                            send_sem=sib_s.at[s], recv_sem=sib_r.at[s], device_id={"model": sibling}, device_id_type=MESH)

    def q_copy(t):
        return pltpu.make_async_remote_copy(src_ref=qbuf.at[t], dst_ref=zin_hbm.at[t], send_sem=qs_s.at[t], recv_sem=z_r.at[t],
                                            device_id={"model": near}, device_id_type=MESH)

    def x_copy(t):
        return pltpu.make_async_remote_copy(src_ref=qbuf.at[t], dst_ref=xin_hbm.at[t], send_sem=qs_s.at[t], recv_sem=x_r.at[t],
                                            device_id={"model": partner}, device_id_type=MESH)

    def dx_local(t):
        return pltpu.make_async_copy(qbuf.at[t], dx_hbm.at[rows_of(t, core)], dxl_s.at[t])

    def dx_sib(t):
        return pltpu.make_async_remote_copy(src_ref=qbuf.at[t], dst_ref=dx_hbm.at[rows_of(t, core)], send_sem=dxs_s.at[t], recv_sem=dxs_r.at[t],
                                            device_id={"model": sibling}, device_id_type=MESH)

    def dx_out(t):
        return pltpu.make_async_remote_copy(src_ref=qbuf.at[t], dst_ref=dx_hbm.at[rows_of(t, core)], send_sem=dxo_s.at[t], recv_sem=dxo_r.at[t],
                                            device_id={"model": near}, device_id_type=MESH)

    def dx_fwd(t):
        return pltpu.make_async_remote_copy(src_ref=dx_hbm.at[rows_of(t, core)], dst_ref=dx_hbm.at[rows_of(t, core)], send_sem=dxs_s.at[t],
                                            recv_sem=dxs_r.at[t], device_id={"model": sibling}, device_id_type=MESH)

    def z_load(t):
        return pltpu.make_async_copy(zin_hbm.at[t], zst, st_sem.at[0])

    def x_load(t):
        return pltpu.make_async_copy(xin_hbm.at[t], xst, st_sem.at[1])

    def lx_load(t):
        return pltpu.make_async_copy(x_hbm.at[rows_of(t, core)], lx, st_sem.at[2])

    def ly_load(t):
        return pltpu.make_async_copy(dy_hbm.at[rows_of(t, core)], ly, st_sem.at[3])

    def pair_sum(t):
        cp = sib_copy(t)
        cp.wait_send()
        cp.wait_recv()
        for h in range(2):
            own = pst[pl.ds(pl.multiple_of(core * HALF + h * PART, PART), PART), :].astype(F32)
            qbuf[2 * t + h] = (own + sib_in[lax.rem(t, 2), h * PART:(h + 1) * PART, :].astype(F32)).astype(BF16)

            @pl.when(is_out)
            def _(h=h):
                q_copy(2 * t + h).start()

    def e3_fetch(t):
        q_copy(t).wait_recv()
        z_load(t).start()

    def e3_process(t):
        z_load(t).wait()
        qbuf[t] = (qbuf[t].astype(F32) + zst[...].astype(F32)).astype(BF16)
        x_copy(t).start()

    def e4_fetch(t):
        x_copy(t).wait_recv()
        x_load(t).start()
        lx_load(t).start()
        ly_load(t).start()

    def e4_process(t):
        x_load(t).wait()
        lx_load(t).wait()
        ly_load(t).wait()
        x_copy(t).wait_send()
        mean, rstd = row_stats(NB - 1 - t // 2, core * 2 + lax.rem(t, 2))
        xh = (lx[...].astype(F32) - mean) * rstd
        d = (qbuf[t].astype(F32) + xst[...].astype(F32)) * gain[...]
        md = jnp.sum(d, axis=1, keepdims=True) * (1.0 / D)
        mdx = jnp.sum(d * xh, axis=1, keepdims=True) * (1.0 / D)
        qbuf[t] = (ly[...].astype(F32) + rstd * (d - md - xh * mdx)).astype(BF16)
        dx_out(t).start()
        dx_sib(t).start()
        dx_local(t).start()

    def e5(t):
        dx_out(t).wait_recv()
        dx_fwd(t).start()

    def lookup(table, k):
        v = jnp.int32(table[0])
        for at in range(1, len(table)):
            v = jnp.where(k == at, table[at], v)
        return v

    def service_points(table, k):
        start, fire = lookup(table[0], k), lookup(table[1], k)
        c = [start % 64, (start // 64) % 64, (start // 4096) % 64]
        pend = [(start // 262144) % 2, (start // 524288) % 2]
        points = []
        for p in range(table[2]):
            f = [(fire // 2 ** (3 * p + step)) % 2 for step in range(3)]
            points.append((list(c), list(pend), f))
            c = [a + b for a, b in zip(c, f)]
            pend = f[:2]
        return points

    def service(point):
        c, pend, f = point

        @pl.when(is_mid & (pend[0] > 0))
        def _():
            e3_process(c[0] - 1)

        @pl.when(is_mid & (f[0] > 0))
        def _():
            e3_fetch(c[0])

        @pl.when(is_mid & (pend[1] > 0))
        def _():
            e4_process(c[1] - 1)

        @pl.when(is_mid & (f[1] > 0))
        def _():
            e4_fetch(c[1])

        @pl.when(is_out & (f[2] > 0))
        def _():
            e5(c[2])

    def row_stats(i, part=None):
        out = []
        for first in (0, NB):
            row = small_ref[pl.ds(first + i, 1), :]
            if part is None:
                col = jnp.broadcast_to(row, (128, R)).T
            else:
                row = jnp.where(part >= 2, row[:, HALF:], row[:, :HALF])
                col = jnp.broadcast_to(row, (128, HALF)).T
                col = jnp.where(lax.rem(part, 2) == 0, col[:PART], col[PART:])
            out.append(jnp.concatenate([col] * (D // 128), axis=1))
        return out

    def rope_of(i):
        cb, sb = cb_ref[pl.ds(i, 1), :], sb_ref[pl.ds(i, 1), :]
        co, so = co_ref[...], so_ref[...]
        return cb * co - sb * so, sb * co + cb * so

    def rope(x, cosf, sinf):
        x0 = x[:, :128]
        lane = lax.broadcasted_iota(jnp.int32, x0.shape, 1)
        other = jnp.where(lane < H // 8, pltpu.roll(x0, 128 - H // 8, 1), pltpu.roll(x0, H // 8, 1))
        return jnp.concatenate([x0 * cosf + other * sinf, x[:, 128:]], axis=1)

    def attention_phase(kv, kT, vv, vT, dk, dv, es, dps, w1, w2, wqkv, wo, nbuf, ybuf, gst, dast, dqkvst, ost, qs, qT, do, doT, oT, dqT, msc, stat):
        w_loads = [pltpu.make_async_copy(s, d_, w_sem.at[k]) for k, (s, d_) in enumerate(((wqkv_hbm, wqkv), (wo_hbm, wo), (w1_hbm, w1), (w2_hbm, w2)))]

        def blk(i):
            return pl.ds(pl.multiple_of(i * R, R), R)

        def x_in(b):
            return pltpu.make_async_copy(x_hbm.at[blk(b)], ybuf.at[lax.rem(b + 1, 2)], in_sem.at[0, lax.rem(b + 1, 2)])

        def n_out(b):
            return pltpu.make_async_copy(nbuf.at[lax.rem(b + 1, 2)], n_hbm.at[blk(b)], out_sem.at[0, lax.rem(b + 1, 2)])

        def n_in(t):
            return pltpu.make_async_copy(n_hbm.at[blk(NB - 1 - t)], nbuf.at[lax.rem(t, 2)], in_sem.at[1, lax.rem(t, 2)])

        def y_in(t):
            return pltpu.make_async_copy(dy_hbm.at[blk(NB - 1 - t)], ybuf.at[lax.rem(t + 1, 2)], in_sem.at[0, lax.rem(t + 1, 2)])

        w_loads[0].start()
        x_in(0).start()
        for w in w_loads[1:]:
            w.start()
        dk[...] = jnp.zeros_like(dk)
        dv[...] = jnp.zeros_like(dv)

        def normed(b):
            slot = lax.rem(b + 1, 2)
            mean, rstd = row_stats(b)
            nbuf[slot] = (((ybuf[slot].astype(F32) - mean) * rstd) * gain[...]).astype(BF16)

        def keys_values(b):
            kvp = mm(nbuf[lax.rem(b + 1, 2)], wqkv[:, H:])
            cosf, sinf = rope_of(b)
            kf = rope(kvp[:, :H], cosf, sinf)
            vf = kvp[:, H:]
            kv[blk(b), :] = kf.astype(BF16)
            vv[blk(b), :] = vf.astype(BF16)
            kT[:, blk(b)] = kf.T.astype(BF16)
            vT[:, blk(b)] = vf.T.astype(BF16)

        x_in(1).start()
        x_in(0).wait()
        normed(0)
        n_out(0).start()
        w_loads[0].wait()

        @pl.loop(0, NB - 1)
        def _(b):
            x_in(b + 1).wait()

            @pl.when(b + 2 < NB)
            def _():
                x_in(b + 2).start()

            @pl.when(b + 2 == NB)
            def _():
                y_in(0).start()

            @pl.when(b >= 1)
            def _():
                n_out(b - 1).wait()

            normed(b + 1)
            keys_values(b)
            n_out(b + 1).start()

        keys_values(NB - 1)
        n_out(NB - 2).wait()
        n_out(NB - 1).wait()

        def outs(t):
            s, i = lax.rem(t, 2), NB - 1 - t
            return [pltpu.make_async_copy(gst.at[s], g_hbm.at[blk(i)], out_sem.at[0, s]),
                    pltpu.make_async_copy(dast.at[s], da_hbm.at[blk(i)], out_sem.at[1, s]),
                    pltpu.make_async_copy(dqkvst.at[s], dqkv_hbm.at[blk(i)], out_sem.at[2, s]),
                    pltpu.make_async_copy(ost.at[s], o_hbm.at[blk(i)], out_sem.at[3, s])]

        for w in w_loads[1:]:
            w.wait()

        @pl.loop(0, NB)
        def _(t):
            slot = lax.rem(t, 2)
            i = NB - 1 - t
            yslot = lax.rem(t + 1, 2)

            @pl.when(t >= 2)
            def _():
                n_in(t).wait()
                for cp in outs(t - 2):
                    cp.wait()

            y_in(t).wait()

            @pl.when((t >= 1) & (t + 1 < NB))
            def _():
                n_in(t + 1).start()

            @pl.when(t + 1 < NB)
            def _():
                y_in(t + 1).start()

            points = service_points(plan[0], t)
            service(points[0])

            FT = min(512, F)
            for f in range(0, F, FT):
                a = mm(nbuf[slot], w1[:, f:f + FT])
                da = mm_nt(ybuf[yslot], w2[f:f + FT, :])
                phi = 0.5 + 0.5 * lax.erf(a * 0.7071067811865476)
                gst[slot, :, f:f + FT] = (a * phi).astype(BF16)
                dast[slot, :, f:f + FT] = (da * (phi + a * (0.3989422804014327 * jnp.exp(-0.5 * (a * a))))).astype(BF16)

            cosf, sinf = rope_of(i)
            qf = rope(mm(nbuf[slot], wqkv[:, :H]), cosf, sinf).astype(BF16).astype(F32) * (H ** -0.5)
            qs[...] = qf.astype(BF16)
            qT[...] = qf.T.astype(BF16)
            dof = mm_nt(ybuf[yslot], wo[...])
            do[...] = dof.astype(BF16)
            doT[...] = dof.T.astype(BF16)
            g_out, da_out, dqkv_out, o_out = outs(t)
            g_out.start()
            da_out.start()

            @pl.when(t > 1)
            def _():
                pair_sum(t - 1)

            service(points[1])

            nfull = i // QPC

            below = jnp.where(lax.broadcasted_iota(jnp.int32, (R, R), 0) <= lax.broadcasted_iota(jnp.int32, (R, R), 1), 0.0, NEG)

            def part(j, u, n=1):
                return pl.ds(pl.multiple_of(j * C + u * R, R), n * R)

            def pass_a(j, carry, subs, diagonal):
                m, l, dl = carry
                for u in range(subs):
                    st = mm(kv[part(j, u), :], qT[...])
                    if diagonal and u == subs - 1:
                        st = jnp.where(below == 0.0, st, NEG)
                    dp = mm(vv[part(j, u), :], doT[...])
                    m_new = jnp.maximum(m, jnp.max(st, axis=0, keepdims=True))
                    alpha = jnp.exp(m - m_new)
                    e = jnp.exp(st - m_new)
                    es[part(j, u), :] = e
                    dps[part(j, u), :] = dp
                    msc[pl.ds(j * QPC + u, 1), :] = m_new
                    m, l, dl = m_new, l * alpha + jnp.sum(e, axis=0, keepdims=True), dl * alpha + jnp.sum(e * dp, axis=0, keepdims=True)
                return m, l, dl

            init = (jnp.full((1, R), NEG, F32), jnp.zeros((1, R), F32), jnp.zeros((1, R), F32))
            carry = lax.fori_loop(0, nfull, functools.partial(pass_a, subs=QPC, diagonal=False), init)
            for row, value in enumerate(carry):
                stat[row:row + 1, :] = value
            for v in range(QPC):
                @pl.when(lax.rem(i, QPC) == v)
                def _(v=v):
                    carry = pass_a(nfull, tuple(stat[row:row + 1, :] for row in range(3)), v + 1, True)
                    for row, value in enumerate(carry):
                        stat[row:row + 1, :] = value

            service(points[2])
            m = stat[0:1, :]
            inv_l = 1.0 / stat[1:2, :]
            delta = stat[2:3, :] * inv_l
            oT[...] = jnp.zeros_like(oT)
            dqT[...] = jnp.zeros_like(dqT)

            def pass_b(j, subs):
                pbs, dss = [], []
                for u in range(subs):
                    p = es[part(j, u), :] * (jnp.exp(msc[pl.ds(j * QPC + u, 1), :] - m) * inv_l)
                    pbs.append(p.astype(BF16))
                    dss.append((p * (dps[part(j, u), :] - delta)).astype(BF16))
                pb, ds = jnp.concatenate(pbs, axis=0), jnp.concatenate(dss, axis=0)
                keys = part(j, 0, subs)
                oT[...] += mm(vT[:, keys], pb)
                dqT[...] += mm(kT[:, keys], ds)
                dv[keys, :] += mm(pb, do[...])
                dk[keys, :] += mm(ds, qs[...])

            @pl.loop(0, nfull)
            def _(j):
                pass_b(j, QPC)

            for v in range(QPC):
                @pl.when(lax.rem(i, QPC) == v)
                def _(v=v):
                    pass_b(nfull, v + 1)

            service(points[3])

            EARLY = min(4 * R, T, D)
            for c in range(0, EARLY, R):
                es[c:c + R, :] = mm_nt(dast[slot], w1[c:c + R, :])

            ost[slot] = oT[...].T.astype(BF16)
            dqkvst[slot, :, :H] = rope(dqT[...].T * (H ** -0.5), cosf, -sinf).astype(BF16)
            dqkvst[slot, :, H:2 * H] = rope(dk[blk(i), :], cosf, -sinf).astype(BF16)
            dqkvst[slot, :, 2 * H:] = dv[blk(i), :].astype(BF16)
            dqkv_out.start()
            o_out.start()

            DT = min(512, D)
            for c in range(0, EARLY, R):
                pst[:, c:c + R] = (es[c:c + R, :] + mm_nt(dqkvst[slot], wqkv[c:c + R, :])).astype(BF16)
            for c in range(EARLY, D, DT):
                pst[:, c:c + DT] = (mm_nt(dast[slot], w1[c:c + DT, :]) + mm_nt(dqkvst[slot], wqkv[c:c + DT, :])).astype(BF16)
            sib_copy(t).start()

            @pl.when(t == 0)
            def _():
                pair_sum(0)

        for t in (NB - 2, NB - 1):
            for cp in outs(t):
                cp.wait()

    pl.run_scoped(
        attention_phase,
        pltpu.VMEM((T, H), BF16), pltpu.VMEM((H, T), BF16), pltpu.VMEM((T, H), BF16), pltpu.VMEM((H, T), BF16),
        pltpu.VMEM((T, H), F32), pltpu.VMEM((T, H), F32), pltpu.VMEM((T, R), F32), pltpu.VMEM((T, R), F32),
        pltpu.VMEM((D, F), BF16), pltpu.VMEM((F, D), BF16), pltpu.VMEM((D, 3 * H), BF16), pltpu.VMEM((H, D), BF16),
        pltpu.VMEM((2, R, D), BF16), pltpu.VMEM((2, R, D), BF16), pltpu.VMEM((2, R, F), BF16), pltpu.VMEM((2, R, F), BF16),
        pltpu.VMEM((2, R, 3 * H), BF16), pltpu.VMEM((2, R, H), BF16),
        pltpu.VMEM((R, H), BF16), pltpu.VMEM((H, R), BF16), pltpu.VMEM((R, H), BF16), pltpu.VMEM((H, R), BF16),
        pltpu.VMEM((H, R), F32), pltpu.VMEM((H, R), F32), pltpu.VMEM((max(8, NB), R), F32), pltpu.VMEM((8, R), F32))

    NT1, NT2 = D // H, F // H

    def weight_phase(da, dqkv, dy, nt, w1st, wqst, w2st):
        loads = [pltpu.make_async_copy(s, d_, w_sem.at[k]) for k, (s, d_) in enumerate(((da_hbm, da), (dqkv_hbm, dqkv), (dy_hbm, dy)))]

        def cols(m):
            return pl.ds(pl.multiple_of(m * H, H), H)

        def nt_in(m):
            return pltpu.make_async_copy(n_hbm.at[:, cols(m)], nt.at[lax.rem(m, 2)], t2_sem.at[0, lax.rem(m, 2)])

        def g_in(m):
            return pltpu.make_async_copy(g_hbm.at[:, cols(m)], nt.at[lax.rem(m, 2)], t2_sem.at[0, lax.rem(m, 2)])

        def o_in():
            return pltpu.make_async_copy(o_hbm, nt.at[NT2 % 2], t2_sem.at[0, NT2 % 2])

        def out1(m):
            s = lax.rem(m, 2)
            return [pltpu.make_async_copy(w1st.at[s], dw1_hbm.at[cols(m)], t2_sem.at[1, s]),
                    pltpu.make_async_copy(wqst.at[s], dwqkv_hbm.at[cols(m)], t2_sem.at[2, s])]

        def out2(m):
            return pltpu.make_async_copy(w2st.at[lax.rem(m, 2)], dw2_hbm.at[cols(m)], t2_sem.at[1, lax.rem(m, 2)])

        def out3():
            return pltpu.make_async_copy(w2st.at[NT2 % 2], dwo_hbm, t2_sem.at[1, NT2 % 2])

        nt_in(0).start()
        loads[1].start()
        loads[0].start()
        loads[2].start()
        pair_sum(NB - 1)

        @pl.loop(0, NT1)
        def _(m):
            s = lax.rem(m, 2)
            nt_in(m).wait()

            @pl.when(m + 1 < NT1)
            def _():
                nt_in(m + 1).start()

            @pl.when(m + 1 == NT1)
            def _():
                g_in(0).start()

            @pl.when(m >= 2)
            def _():
                for cp in out1(m - 2):
                    cp.wait()

            points = service_points(plan[1], m)
            service(points[0])

            @pl.when(m == 0)
            def _():
                loads[1].wait()

            wqst[s] = mm_tn(nt[s], dqkv[...]).astype(BF16)
            service(points[1])

            @pl.when(m == 0)
            def _():
                loads[0].wait()

            w1st[s] = mm_tn(nt[s], da[...]).astype(BF16)
            for cp in out1(m):
                cp.start()

        for m in (NT1 - 2, NT1 - 1):
            for cp in out1(m):
                cp.wait()
        loads[2].wait()

        @pl.loop(0, NT2)
        def _(m):
            s = lax.rem(m, 2)
            g_in(m).wait()

            @pl.when(m + 1 < NT2)
            def _():
                g_in(m + 1).start()

            @pl.when(m + 1 == NT2)
            def _():
                o_in().start()

            @pl.when(m >= 2)
            def _():
                out2(m - 2).wait()

            points = service_points(plan[1], NT1 + m)
            service(points[0])
            w2st[s, :, :D // 2] = mm_tn(nt[s], dy[:, :D // 2]).astype(BF16)
            service(points[1])
            w2st[s, :, D // 2:] = mm_tn(nt[s], dy[:, D // 2:]).astype(BF16)
            out2(m).start()

        o_in().wait()
        out2(NT2 - 2).wait()
        points = service_points(plan[1], NT1 + NT2)
        service(points[0])
        w2st[NT2 % 2, :, :D // 2] = mm_tn(nt[NT2 % 2], dy[:, :D // 2]).astype(BF16)
        service(points[1])
        w2st[NT2 % 2, :, D // 2:] = mm_tn(nt[NT2 % 2], dy[:, D // 2:]).astype(BF16)
        out3().start()
        out2(NT2 - 1).wait()
        out3().wait()

    pl.run_scoped(
        weight_phase,
        pltpu.VMEM((T, F), BF16), pltpu.VMEM((T, 3 * H), BF16), pltpu.VMEM((T, D), BF16), pltpu.VMEM((2, T, H), BF16),
        pltpu.VMEM((2, H, F), BF16), pltpu.VMEM((2, H, 3 * H), BF16), pltpu.VMEM((2, H, D), BF16))

    (l3, l4, l5), last3, last4 = plan[2]
    service(([l3, l4, l5], [jnp.int32(last3), jnp.int32(last4)], [jnp.int32(0)] * 3))

    @pl.when(is_mid)
    def _():
        @pl.loop(0, NS - l4)
        def _(k):
            @pl.when(l3 + k < NS)
            def _():
                e3_fetch(l3 + k)
                e3_process(l3 + k)

            e4_fetch(l4 + k)
            e4_process(l4 + k)

        @pl.loop(0, NS)
        def _(t):
            dx_local(t).wait()
            dx_sib(t).wait_send()
            dx_out(t).wait_send()
            dx_sib(t).wait_recv()

    @pl.when(is_out)
    def _():
        @pl.loop(l5, NS)
        def _(t):
            e5(t)

        @pl.loop(0, NS)
        def _(t):
            q_copy(t).wait_send()
            dx_fwd(t).wait_send()
            dx_fwd(t).wait_recv()


def service_plan(blocks, tiles):
    wire, lat, slow, count = 5.65, 2.5, 1.08, 2 * blocks
    at, ready, now = [], [], 20.5
    for t in range(blocks):
        keys = blocks - t
        mlp = now + 3.6
        at += [now, mlp, mlp + 0.4 + 0.14 * keys * slow, mlp + 0.8 + 0.32 * keys * slow]
        if t > 1:
            ready += [mlp, mlp]
        now = at[-1] + 3.0
        if t == 0:
            now += 2.0
            ready += [now, now]
    ready += [now + 0.5, now + 0.5]
    now += 4.0
    for m in range(tiles):
        at += [now, now + 2.3]
        now += 5.0
    at.append(now)
    fires = []
    for step in range(3):
        table, sent, free, k = [], [], 0.0, 0
        for t in range(count):
            free = max(free, ready[t]) + wire
            while k < len(at) - 1 and at[k] < free + lat:
                k += 1
            if k < len(at) - 1:
                table.append(k)
                sent.append(at[k + 1])
                k += 1
            else:
                sent.append(free + lat)
        fires.append(set(table))
        ready = sent
    done, last, tables = [0, 0, 0], [0, 0], []
    k = 0
    for units, points in ((blocks, 4), (tiles, 2)):
        starts, codes = [], []
        for _ in range(units):
            starts.append(done[0] + 64 * done[1] + 4096 * done[2] + 262144 * last[0] + 524288 * last[1])
            code = 0
            for p in range(points):
                f = [int(k in fire) for fire in fires]
                code += sum(v * 2 ** (3 * p + step) for step, v in enumerate(f))
                done = [a + b for a, b in zip(done, f)]
                last = f[:2]
                k += 1
            codes.append(code)
        tables.append((tuple(starts), tuple(codes), points))
    return tables[0], tables[1], (tuple(done), last[0], last[1])


def copy_kernel(*refs):
    n = len(refs) // 4
    pieces = []
    for src, dst, buf, sem in zip(refs[:n], refs[n:2 * n], refs[2 * n:3 * n], refs[3 * n:]):
        count = sem.shape[1]
        rows = src.shape[0] // count
        for p in range(count):
            part = pl.ds(p * rows, rows)
            pieces.append((pltpu.make_async_copy(src.at[part], buf.at[part], sem.at[0, p]), pltpu.make_async_copy(buf.at[part], dst.at[part], sem.at[1, p])))
    for load, _ in pieces:
        load.start()
    for load, store in pieces:
        load.wait()
        store.start()
    for _, store in pieces:
        store.wait()


def copy_out(arrays):
    any_spec = pl.BlockSpec(memory_space=pl.ANY)
    counts = [2 ** max(0, (a.size // (512 * 1024)).bit_length() - 1) for a in arrays]
    return pl.pallas_call(
        copy_kernel, name="results",
        out_shape=[jax.ShapeDtypeStruct(a.shape, a.dtype) for a in arrays],
        in_specs=[any_spec] * len(arrays), out_specs=[any_spec] * len(arrays),
        scratch_shapes=[pltpu.VMEM(a.shape, a.dtype) for a in arrays] + [pltpu.SemaphoreType.DMA((2, c)) for c in counts],
        compiler_params=pltpu.CompilerParams(vmem_limit_bytes=67043328))(*arrays)


def rope_tables(blocks, head_dim):
    rot = head_dim // 4
    half = rot // 2
    inv_freq = np.power(np.float32(10000.0), (-2.0 * np.arange(half, dtype=np.float32) / rot).astype(np.float32)).astype(np.float64)
    freq = np.zeros((1, 128))
    freq[0, :half], freq[0, half:rot] = -inv_freq, inv_freq
    at = np.arange(blocks)[:, None] * ROWS * freq
    off = np.arange(ROWS)[:, None] * freq
    return [np.asarray(t, np.float32) for t in (np.cos(at), np.sin(at), np.cos(off), np.sin(off))]


def solution(mesh):
    def device_step(resid_x, ln_mean, ln_rstd, ln_gain, grad_y, w_qkv, w_out, w_up, w_down):
        T, D = resid_x.shape
        F = w_up.shape[1]
        H = w_out.shape[1]
        NB = T // ROWS
        HALF = ROWS // 2
        C = min(1024, T)
        tabs = [jnp.asarray(t) for t in rope_tables(NB, H)]
        small = jnp.concatenate([ln_mean, ln_rstd, ln_gain.astype(F32)]).reshape(2 * NB + D // ROWS, ROWS)
        any_spec = pl.BlockSpec(memory_space=pl.ANY)
        vmem = pl.BlockSpec(memory_space=pltpu.VMEM)
        sds = lambda *s: jax.ShapeDtypeStruct(s, BF16)
        outs = pl.pallas_call(
            functools.partial(layer_kernel, (T, D, F, H, C), service_plan(NB, D // H + F // H + 1)),
            name="layer_backward",
            out_shape=[sds(T, D), sds(D, 3 * H), sds(H, D), sds(D, F), sds(F, D),
                       sds(T, D), sds(T, F), sds(T, F), sds(T, 3 * H), sds(T, H), sds(2 * NB, HALF // 2, D), sds(2 * NB, HALF // 2, D)],
            in_specs=[any_spec, any_spec] + [vmem] * 5 + [any_spec, any_spec, any_spec, any_spec],
            out_specs=[any_spec] * 12,
            scratch_shapes=[
                pltpu.VMEM((1, D), F32), pltpu.VMEM((2 * NB, HALF // 2, D), BF16), pltpu.VMEM((ROWS, D), BF16), pltpu.VMEM((2, HALF, D), BF16),
                *[pltpu.VMEM((HALF // 2, D), BF16)] * 4,
                pltpu.SemaphoreType.DMA((2,)), pltpu.SemaphoreType.DMA((2,))]
            + [pltpu.SemaphoreType.DMA((2 * NB,))] * 8
            + [pltpu.SemaphoreType.DMA((4,)), pltpu.SemaphoreType.DMA((2, 2)), pltpu.SemaphoreType.DMA((4,)), pltpu.SemaphoreType.DMA((4, 2)),
               pltpu.SemaphoreType.DMA((3, 2))],
            compiler_params=pltpu.CompilerParams(collective_id=0, has_side_effects=True, vmem_limit_bytes=67043328),
        )(resid_x, grad_y, small, *tabs, w_qkv, w_out.reshape(H, D), w_up, w_down)
        grad_x, grad_w_qkv, grad_w_out, grad_w_up, grad_w_down = copy_out(outs[:5])
        return grad_x, grad_w_qkv, grad_w_out.reshape(1, H, D), grad_w_up, grad_w_down

    in_specs = (P("data", None), P("data"), P("data"), P(None), P("data", None), P(None, "model"), P("model", None, None), P(None, "model"), P("model", None))
    out_specs = (P("data", None), P("data", "model"), P(("data", "model"), None, None), P("data", "model"), P(("data", "model"), None))
    return jax.shard_map(device_step, mesh=mesh, in_specs=in_specs, out_specs=out_specs, check_vma=False)
```

```python
import functools

import jax
import jax.numpy as jnp
import numpy as np
from jax import lax
from jax.experimental import pallas as pl
from jax.experimental.pallas import tpu as pltpu
from jax.sharding import PartitionSpec as P

MESH = pl.DeviceIdType.MESH
F32, BF16 = jnp.float32, jnp.bfloat16
ROWS = 256
NEG = -1e30


def mm(a, b):
    return jnp.dot(a, b, preferred_element_type=F32)


def mm_nt(a, b):
    return lax.dot_general(a, b, (((1,), (1,)), ((), ())), preferred_element_type=F32)


def mm_tn(a, b):
    return lax.dot_general(a, b, (((0,), (0,)), ((), ())), preferred_element_type=F32)


def clip(v, hi):
    return jnp.minimum(jnp.maximum(v, 0), hi)


def layer_kernel(dims, plan, x_hbm, dy_hbm, small_ref, cb_ref, sb_ref, co_ref, so_ref, wqkv_hbm, wo_hbm, w1_hbm, w2_hbm,
                 dx_hbm, dwqkv_hbm, dwo_hbm, dw1_hbm, dw2_hbm, n_hbm, g_hbm, da_hbm, dqkv_hbm, o_hbm, zin_hbm, xin_hbm,
                 gain, qbuf, pst, sib_in, zst, xst, lx, ly,
                 sib_s, sib_r, qs_s, z_r, x_r, dxl_s, dxs_s, dxo_s, dxo_r, dxs_r, st_sem, in_sem, w_sem, out_sem, t2_sem):
    T, D, F, H, C = dims
    R = ROWS
    HALF = R // 2
    PART = HALF // 2
    NB = T // R
    NS = 2 * NB
    QPC = C // R
    me = lax.axis_index("model")
    core = lax.rem(me, 2)
    z = me // 2
    nbz = z + 1 - 2 * lax.rem(z, 2)
    sibling = z * 2 + 1 - core
    near = nbz * 2 + core
    partner = (3 - z) * 2 + core
    is_mid = (z == 1) | (z == 2)
    is_out = (z == 0) | (z == 3)

    for c in range(D // R):
        gain[:, c * R:(c + 1) * R] = small_ref[2 * NB + c:2 * NB + c + 1, :]
    barrier = pltpu.get_barrier_semaphore()
    pl.semaphore_signal(barrier, inc=1, device_id={"model": sibling}, device_id_type=MESH)
    pl.semaphore_signal(barrier, inc=1, device_id={"model": near}, device_id_type=MESH)

    @pl.when(is_mid)
    def _():
        pl.semaphore_signal(barrier, inc=1, device_id={"model": partner}, device_id_type=MESH)
        pl.semaphore_wait(barrier, 3)

    @pl.when(is_out)
    def _():
        pl.semaphore_wait(barrier, 2)

    def rows_of(t, c):
        return pl.ds(pl.multiple_of((NB - 1 - t // 2) * R + c * HALF + lax.rem(t, 2) * PART, PART), PART)

    def sib_copy(t):
        s = lax.rem(t, 2)
        return pltpu.make_async_remote_copy(src_ref=pst.at[pl.ds(pl.multiple_of((1 - core) * HALF, HALF), HALF)], dst_ref=sib_in.at[s],
                                            send_sem=sib_s.at[s], recv_sem=sib_r.at[s], device_id={"model": sibling}, device_id_type=MESH)

    def q_copy(t):
        return pltpu.make_async_remote_copy(src_ref=qbuf.at[t], dst_ref=zin_hbm.at[t], send_sem=qs_s.at[t], recv_sem=z_r.at[t],
                                            device_id={"model": near}, device_id_type=MESH)

    def x_copy(t):
        return pltpu.make_async_remote_copy(src_ref=qbuf.at[t], dst_ref=xin_hbm.at[t], send_sem=qs_s.at[t], recv_sem=x_r.at[t],
                                            device_id={"model": partner}, device_id_type=MESH)

    def dx_local(t):
        return pltpu.make_async_copy(qbuf.at[t], dx_hbm.at[rows_of(t, core)], dxl_s.at[t])

    def dx_sib(t):
        return pltpu.make_async_remote_copy(src_ref=qbuf.at[t], dst_ref=dx_hbm.at[rows_of(t, core)], send_sem=dxs_s.at[t], recv_sem=dxs_r.at[t],
                                            device_id={"model": sibling}, device_id_type=MESH)

    def dx_out(t):
        return pltpu.make_async_remote_copy(src_ref=qbuf.at[t], dst_ref=dx_hbm.at[rows_of(t, core)], send_sem=dxo_s.at[t], recv_sem=dxo_r.at[t],
                                            device_id={"model": near}, device_id_type=MESH)

    def dx_fwd(t):
        return pltpu.make_async_remote_copy(src_ref=dx_hbm.at[rows_of(t, core)], dst_ref=dx_hbm.at[rows_of(t, core)], send_sem=dxs_s.at[t],
                                            recv_sem=dxs_r.at[t], device_id={"model": sibling}, device_id_type=MESH)

    def z_load(t):
        return pltpu.make_async_copy(zin_hbm.at[t], zst, st_sem.at[0])

    def x_load(t):
        return pltpu.make_async_copy(xin_hbm.at[t], xst, st_sem.at[1])

    def lx_load(t):
        return pltpu.make_async_copy(x_hbm.at[rows_of(t, core)], lx, st_sem.at[2])

    def ly_load(t):
        return pltpu.make_async_copy(dy_hbm.at[rows_of(t, core)], ly, st_sem.at[3])

    def pair_sum(t):
        cp = sib_copy(t)
        cp.wait_send()
        cp.wait_recv()
        for h in range(2):
            own = pst[pl.ds(pl.multiple_of(core * HALF + h * PART, PART), PART), :].astype(F32)
            qbuf[2 * t + h] = (own + sib_in[lax.rem(t, 2), h * PART:(h + 1) * PART, :].astype(F32)).astype(BF16)

            @pl.when(is_out)
            def _(h=h):
                q_copy(2 * t + h).start()

    def e3_fetch(t):
        q_copy(t).wait_recv()
        z_load(t).start()

    def e3_process(t):
        z_load(t).wait()
        qbuf[t] = (qbuf[t].astype(F32) + zst[...].astype(F32)).astype(BF16)
        x_copy(t).start()

    def e4_fetch(t):
        x_copy(t).wait_recv()
        x_load(t).start()
        lx_load(t).start()
        ly_load(t).start()

    def e4_process(t):
        x_load(t).wait()
        lx_load(t).wait()
        ly_load(t).wait()
        x_copy(t).wait_send()
        mean, rstd = row_stats(NB - 1 - t // 2, core * 2 + lax.rem(t, 2))
        xh = (lx[...].astype(F32) - mean) * rstd
        d = (qbuf[t].astype(F32) + xst[...].astype(F32)) * gain[...]
        md = jnp.sum(d, axis=1, keepdims=True) * (1.0 / D)
        mdx = jnp.sum(d * xh, axis=1, keepdims=True) * (1.0 / D)
        qbuf[t] = (ly[...].astype(F32) + rstd * (d - md - xh * mdx)).astype(BF16)
        dx_out(t).start()
        dx_sib(t).start()
        dx_local(t).start()

    def e5(t):
        dx_out(t).wait_recv()
        dx_fwd(t).start()

    def lookup(table, k):
        v = jnp.int32(table[0])
        for at in range(1, len(table)):
            v = jnp.where(k == at, table[at], v)
        return v

    def service_points(table, k):
        start, fire = lookup(table[0], k), lookup(table[1], k)
        c = [start % 64, (start // 64) % 64, (start // 4096) % 64]
        pend = [(start // 262144) % 2, (start // 524288) % 2]
        points = []
        for p in range(table[2]):
            f = [(fire // 2 ** (3 * p + step)) % 2 for step in range(3)]
            points.append((list(c), list(pend), f))
            c = [a + b for a, b in zip(c, f)]
            pend = f[:2]
        return points

    def service(point):
        c, pend, f = point

        @pl.when(is_mid & (pend[0] > 0))
        def _():
            e3_process(c[0] - 1)

        @pl.when(is_mid & (f[0] > 0))
        def _():
            e3_fetch(c[0])

        @pl.when(is_mid & (pend[1] > 0))
        def _():
            e4_process(c[1] - 1)

        @pl.when(is_mid & (f[1] > 0))
        def _():
            e4_fetch(c[1])

        @pl.when(is_out & (f[2] > 0))
        def _():
            e5(c[2])

    def row_stats(i, part=None):
        out = []
        for first in (0, NB):
            row = small_ref[pl.ds(first + i, 1), :]
            if part is None:
                col = jnp.broadcast_to(row, (128, R)).T
            else:
                row = jnp.where(part >= 2, row[:, HALF:], row[:, :HALF])
                col = jnp.broadcast_to(row, (128, HALF)).T
                col = jnp.where(lax.rem(part, 2) == 0, col[:PART], col[PART:])
            out.append(jnp.concatenate([col] * (D // 128), axis=1))
        return out

    def rope_of(i):
        cb, sb = cb_ref[pl.ds(i, 1), :], sb_ref[pl.ds(i, 1), :]
        co, so = co_ref[...], so_ref[...]
        return cb * co - sb * so, sb * co + cb * so

    def rope(x, cosf, sinf):
        x0 = x[:, :128]
        lane = lax.broadcasted_iota(jnp.int32, x0.shape, 1)
        other = jnp.where(lane < H // 8, pltpu.roll(x0, 128 - H // 8, 1), pltpu.roll(x0, H // 8, 1))
        return jnp.concatenate([x0 * cosf + other * sinf, x[:, 128:]], axis=1)

    def attention_phase(kv, kT, vv, vT, dk, dv, es, dps, w1, w2, wqkv, wo, nbuf, ybuf, gst, dast, dqkvst, ost, qs, qT, do, doT, oT, dqT, msc, stat):
        w_loads = [pltpu.make_async_copy(s, d_, w_sem.at[k]) for k, (s, d_) in enumerate(((wqkv_hbm, wqkv), (wo_hbm, wo), (w1_hbm, w1), (w2_hbm, w2)))]

        def blk(i):
            return pl.ds(pl.multiple_of(i * R, R), R)

        def x_in(b):
            return pltpu.make_async_copy(x_hbm.at[blk(b)], ybuf.at[lax.rem(b + 1, 2)], in_sem.at[0, lax.rem(b + 1, 2)])

        def n_out(b):
            return pltpu.make_async_copy(nbuf.at[lax.rem(b + 1, 2)], n_hbm.at[blk(b)], out_sem.at[0, lax.rem(b + 1, 2)])

        def n_in(t):
            return pltpu.make_async_copy(n_hbm.at[blk(NB - 1 - t)], nbuf.at[lax.rem(t, 2)], in_sem.at[1, lax.rem(t, 2)])

        def y_in(t):
            return pltpu.make_async_copy(dy_hbm.at[blk(NB - 1 - t)], ybuf.at[lax.rem(t + 1, 2)], in_sem.at[0, lax.rem(t + 1, 2)])

        w_loads[0].start()
        x_in(0).start()
        for w in w_loads[1:]:
            w.start()
        dk[...] = jnp.zeros_like(dk)
        dv[...] = jnp.zeros_like(dv)

        def normed(b):
            slot = lax.rem(b + 1, 2)
            mean, rstd = row_stats(b)
            nbuf[slot] = (((ybuf[slot].astype(F32) - mean) * rstd) * gain[...]).astype(BF16)

        def keys_values(b):
            kvp = mm(nbuf[lax.rem(b + 1, 2)], wqkv[:, H:])
            cosf, sinf = rope_of(b)
            kf = rope(kvp[:, :H], cosf, sinf)
            vf = kvp[:, H:]
            kv[blk(b), :] = kf.astype(BF16)
            vv[blk(b), :] = vf.astype(BF16)
            kT[:, blk(b)] = kf.T.astype(BF16)
            vT[:, blk(b)] = vf.T.astype(BF16)

        x_in(1).start()
        x_in(0).wait()
        normed(0)
        n_out(0).start()
        w_loads[0].wait()

        @pl.loop(0, NB - 1)
        def _(b):
            x_in(b + 1).wait()

            @pl.when(b + 2 < NB)
            def _():
                x_in(b + 2).start()

            @pl.when(b + 2 == NB)
            def _():
                y_in(0).start()

            @pl.when(b >= 1)
            def _():
                n_out(b - 1).wait()

            normed(b + 1)
            keys_values(b)
            n_out(b + 1).start()

        keys_values(NB - 1)
        n_out(NB - 2).wait()
        n_out(NB - 1).wait()

        def outs(t):
            s, i = lax.rem(t, 2), NB - 1 - t
            return [pltpu.make_async_copy(gst.at[s], g_hbm.at[blk(i)], out_sem.at[0, s]),
                    pltpu.make_async_copy(dast.at[s], da_hbm.at[blk(i)], out_sem.at[1, s]),
                    pltpu.make_async_copy(dqkvst.at[s], dqkv_hbm.at[blk(i)], out_sem.at[2, s]),
                    pltpu.make_async_copy(ost.at[s], o_hbm.at[blk(i)], out_sem.at[3, s])]

        for w in w_loads[1:]:
            w.wait()

        @pl.loop(0, NB)
        def _(t):
            slot = lax.rem(t, 2)
            i = NB - 1 - t
            yslot = lax.rem(t + 1, 2)

            @pl.when(t >= 2)
            def _():
                n_in(t).wait()
                for cp in outs(t - 2):
                    cp.wait()

            y_in(t).wait()

            @pl.when((t >= 1) & (t + 1 < NB))
            def _():
                n_in(t + 1).start()

            @pl.when(t + 1 < NB)
            def _():
                y_in(t + 1).start()

            points = service_points(plan[0], t)
            service(points[0])

            FT = min(512, F)
            for f in range(0, F, FT):
                a = mm(nbuf[slot], w1[:, f:f + FT])
                da = mm_nt(ybuf[yslot], w2[f:f + FT, :])
                phi = 0.5 + 0.5 * lax.erf(a * 0.7071067811865476)
                gst[slot, :, f:f + FT] = (a * phi).astype(BF16)
                dast[slot, :, f:f + FT] = (da * (phi + a * (0.3989422804014327 * jnp.exp(-0.5 * (a * a))))).astype(BF16)

            cosf, sinf = rope_of(i)
            qf = rope(mm(nbuf[slot], wqkv[:, :H]), cosf, sinf).astype(BF16).astype(F32) * (H ** -0.5)
            qs[...] = qf.astype(BF16)
            qT[...] = qf.T.astype(BF16)
            dof = mm_nt(ybuf[yslot], wo[...])
            do[...] = dof.astype(BF16)
            doT[...] = dof.T.astype(BF16)
            g_out, da_out, dqkv_out, o_out = outs(t)
            g_out.start()
            da_out.start()

            @pl.when(t > 1)
            def _():
                pair_sum(t - 1)

            service(points[1])

            nfull = i // QPC

            below = jnp.where(lax.broadcasted_iota(jnp.int32, (R, R), 0) <= lax.broadcasted_iota(jnp.int32, (R, R), 1), 0.0, NEG)

            def part(j, u, n=1):
                return pl.ds(pl.multiple_of(j * C + u * R, R), n * R)

            def pass_a(j, carry, subs, diagonal):
                m, l, dl = carry
                for u in range(subs):
                    st = mm(kv[part(j, u), :], qT[...])
                    if diagonal and u == subs - 1:
                        st = jnp.where(below == 0.0, st, NEG)
                    dp = mm(vv[part(j, u), :], doT[...])
                    m_new = jnp.maximum(m, jnp.max(st, axis=0, keepdims=True))
                    alpha = jnp.exp(m - m_new)
                    e = jnp.exp(st - m_new)
                    es[part(j, u), :] = e
                    dps[part(j, u), :] = dp
                    msc[pl.ds(j * QPC + u, 1), :] = m_new
                    m, l, dl = m_new, l * alpha + jnp.sum(e, axis=0, keepdims=True), dl * alpha + jnp.sum(e * dp, axis=0, keepdims=True)
                return m, l, dl

            init = (jnp.full((1, R), NEG, F32), jnp.zeros((1, R), F32), jnp.zeros((1, R), F32))
            carry = lax.fori_loop(0, nfull, functools.partial(pass_a, subs=QPC, diagonal=False), init)
            for row, value in enumerate(carry):
                stat[row:row + 1, :] = value
            for v in range(QPC):
                @pl.when(lax.rem(i, QPC) == v)
                def _(v=v):
                    carry = pass_a(nfull, tuple(stat[row:row + 1, :] for row in range(3)), v + 1, True)
                    for row, value in enumerate(carry):
                        stat[row:row + 1, :] = value

            service(points[2])
            m = stat[0:1, :]
            inv_l = 1.0 / stat[1:2, :]
            delta = stat[2:3, :] * inv_l
            oT[...] = jnp.zeros_like(oT)
            dqT[...] = jnp.zeros_like(dqT)

            def pass_b(j, subs):
                pbs, dss = [], []
                for u in range(subs):
                    p = es[part(j, u), :] * (jnp.exp(msc[pl.ds(j * QPC + u, 1), :] - m) * inv_l)
                    pbs.append(p.astype(BF16))
                    dss.append((p * (dps[part(j, u), :] - delta)).astype(BF16))
                pb, ds = jnp.concatenate(pbs, axis=0), jnp.concatenate(dss, axis=0)
                keys = part(j, 0, subs)
                oT[...] += mm(vT[:, keys], pb)
                dqT[...] += mm(kT[:, keys], ds)
                dv[keys, :] += mm(pb, do[...])
                dk[keys, :] += mm(ds, qs[...])

            @pl.loop(0, nfull)
            def _(j):
                pass_b(j, QPC)

            for v in range(QPC):
                @pl.when(lax.rem(i, QPC) == v)
                def _(v=v):
                    pass_b(nfull, v + 1)

            service(points[3])

            EARLY = min(4 * R, T, D)
            for c in range(0, EARLY, R):
                es[c:c + R, :] = mm_nt(dast[slot], w1[c:c + R, :])

            ost[slot] = oT[...].T.astype(BF16)
            dqkvst[slot, :, :H] = rope(dqT[...].T * (H ** -0.5), cosf, -sinf).astype(BF16)
            dqkvst[slot, :, H:2 * H] = rope(dk[blk(i), :], cosf, -sinf).astype(BF16)
            dqkvst[slot, :, 2 * H:] = dv[blk(i), :].astype(BF16)
            dqkv_out.start()
            o_out.start()

            DT = min(512, D)
            for c in range(0, EARLY, R):
                pst[:, c:c + R] = (es[c:c + R, :] + mm_nt(dqkvst[slot], wqkv[c:c + R, :])).astype(BF16)
            for c in range(EARLY, D, DT):
                pst[:, c:c + DT] = (mm_nt(dast[slot], w1[c:c + DT, :]) + mm_nt(dqkvst[slot], wqkv[c:c + DT, :])).astype(BF16)
            sib_copy(t).start()

            @pl.when(t == 0)
            def _():
                pair_sum(0)

        for t in (NB - 2, NB - 1):
            for cp in outs(t):
                cp.wait()

    pl.run_scoped(
        attention_phase,
        pltpu.VMEM((T, H), BF16), pltpu.VMEM((H, T), BF16), pltpu.VMEM((T, H), BF16), pltpu.VMEM((H, T), BF16),
        pltpu.VMEM((T, H), F32), pltpu.VMEM((T, H), F32), pltpu.VMEM((T, R), F32), pltpu.VMEM((T, R), F32),
        pltpu.VMEM((D, F), BF16), pltpu.VMEM((F, D), BF16), pltpu.VMEM((D, 3 * H), BF16), pltpu.VMEM((H, D), BF16),
        pltpu.VMEM((2, R, D), BF16), pltpu.VMEM((2, R, D), BF16), pltpu.VMEM((2, R, F), BF16), pltpu.VMEM((2, R, F), BF16),
        pltpu.VMEM((2, R, 3 * H), BF16), pltpu.VMEM((2, R, H), BF16),
        pltpu.VMEM((R, H), BF16), pltpu.VMEM((H, R), BF16), pltpu.VMEM((R, H), BF16), pltpu.VMEM((H, R), BF16),
        pltpu.VMEM((H, R), F32), pltpu.VMEM((H, R), F32), pltpu.VMEM((max(8, NB), R), F32), pltpu.VMEM((8, R), F32))

    NT1, NT2 = D // H, F // H

    def weight_phase(da, dqkv, dy, nt, w1st, wqst, w2st):
        loads = [pltpu.make_async_copy(s, d_, w_sem.at[k]) for k, (s, d_) in enumerate(((da_hbm, da), (dqkv_hbm, dqkv), (dy_hbm, dy)))]

        def cols(m):
            return pl.ds(pl.multiple_of(m * H, H), H)

        def nt_in(m):
            return pltpu.make_async_copy(n_hbm.at[:, cols(m)], nt.at[lax.rem(m, 2)], t2_sem.at[0, lax.rem(m, 2)])

        def g_in(m):
            return pltpu.make_async_copy(g_hbm.at[:, cols(m)], nt.at[lax.rem(m, 2)], t2_sem.at[0, lax.rem(m, 2)])

        def o_in():
            return pltpu.make_async_copy(o_hbm, nt.at[NT2 % 2], t2_sem.at[0, NT2 % 2])

        def out1(m):
            s = lax.rem(m, 2)
            return [pltpu.make_async_copy(w1st.at[s], dw1_hbm.at[cols(m)], t2_sem.at[1, s]),
                    pltpu.make_async_copy(wqst.at[s], dwqkv_hbm.at[cols(m)], t2_sem.at[2, s])]

        def out2(m):
            return pltpu.make_async_copy(w2st.at[lax.rem(m, 2)], dw2_hbm.at[cols(m)], t2_sem.at[1, lax.rem(m, 2)])

        def out3():
            return pltpu.make_async_copy(w2st.at[NT2 % 2], dwo_hbm, t2_sem.at[1, NT2 % 2])

        nt_in(0).start()
        loads[1].start()
        loads[0].start()
        loads[2].start()
        pair_sum(NB - 1)

        @pl.loop(0, NT1)
        def _(m):
            s = lax.rem(m, 2)
            nt_in(m).wait()

            @pl.when(m + 1 < NT1)
            def _():
                nt_in(m + 1).start()

            @pl.when(m + 1 == NT1)
            def _():
                g_in(0).start()

            @pl.when(m >= 2)
            def _():
                for cp in out1(m - 2):
                    cp.wait()

            points = service_points(plan[1], m)
            service(points[0])

            @pl.when(m == 0)
            def _():
                loads[1].wait()

            wqst[s] = mm_tn(nt[s], dqkv[...]).astype(BF16)
            service(points[1])

            @pl.when(m == 0)
            def _():
                loads[0].wait()

            w1st[s] = mm_tn(nt[s], da[...]).astype(BF16)
            for cp in out1(m):
                cp.start()

        for m in (NT1 - 2, NT1 - 1):
            for cp in out1(m):
                cp.wait()
        loads[2].wait()

        @pl.loop(0, NT2)
        def _(m):
            s = lax.rem(m, 2)
            g_in(m).wait()

            @pl.when(m + 1 < NT2)
            def _():
                g_in(m + 1).start()

            @pl.when(m + 1 == NT2)
            def _():
                o_in().start()

            @pl.when(m >= 2)
            def _():
                out2(m - 2).wait()

            points = service_points(plan[1], NT1 + m)
            service(points[0])
            w2st[s, :, :D // 2] = mm_tn(nt[s], dy[:, :D // 2]).astype(BF16)
            service(points[1])
            w2st[s, :, D // 2:] = mm_tn(nt[s], dy[:, D // 2:]).astype(BF16)
            out2(m).start()

        o_in().wait()
        out2(NT2 - 2).wait()
        points = service_points(plan[1], NT1 + NT2)
        service(points[0])
        w2st[NT2 % 2, :, :D // 2] = mm_tn(nt[NT2 % 2], dy[:, :D // 2]).astype(BF16)
        service(points[1])
        w2st[NT2 % 2, :, D // 2:] = mm_tn(nt[NT2 % 2], dy[:, D // 2:]).astype(BF16)
        out3().start()
        out2(NT2 - 1).wait()
        out3().wait()

    pl.run_scoped(
        weight_phase,
        pltpu.VMEM((T, F), BF16), pltpu.VMEM((T, 3 * H), BF16), pltpu.VMEM((T, D), BF16), pltpu.VMEM((2, T, H), BF16),
        pltpu.VMEM((2, H, F), BF16), pltpu.VMEM((2, H, 3 * H), BF16), pltpu.VMEM((2, H, D), BF16))

    (l3, l4, l5), last3, last4 = plan[2]
    service(([l3, l4, l5], [jnp.int32(last3), jnp.int32(last4)], [jnp.int32(0)] * 3))

    @pl.when(is_mid)
    def _():
        @pl.loop(0, NS - l4)
        def _(k):
            @pl.when(l3 + k < NS)
            def _():
                e3_fetch(l3 + k)
                e3_process(l3 + k)

            e4_fetch(l4 + k)
            e4_process(l4 + k)

        @pl.loop(0, NS)
        def _(t):
            dx_local(t).wait()
            dx_sib(t).wait_send()
            dx_out(t).wait_send()
            dx_sib(t).wait_recv()

    @pl.when(is_out)
    def _():
        @pl.loop(l5, NS)
        def _(t):
            e5(t)

        @pl.loop(0, NS)
        def _(t):
            q_copy(t).wait_send()
            dx_fwd(t).wait_send()
            dx_fwd(t).wait_recv()


def service_plan(blocks, tiles):
    wire, lat, slow, count = 5.65, 2.5, 1.08, 2 * blocks
    at, ready, now = [], [], 20.5
    for t in range(blocks):
        keys = blocks - t
        mlp = now + 3.6
        at += [now, mlp, mlp + 0.4 + 0.14 * keys * slow, mlp + 0.8 + 0.32 * keys * slow]
        if t > 1:
            ready += [mlp, mlp]
        now = at[-1] + 3.0
        if t == 0:
            now += 2.0
            ready += [now, now]
    ready += [now + 0.5, now + 0.5]
    now += 5.0
    for m in range(tiles):
        at += [now, now + 2.6]
        now += 5.4
    at.append(now)
    fires = []
    for step in range(3):
        table, sent, free, k = [], [], 0.0, 0
        for t in range(count):
            free = max(free, ready[t]) + wire
            while k < len(at) - 1 and at[k] < free + lat:
                k += 1
            if k < len(at) - 1:
                table.append(k)
                sent.append(at[k + 1])
                k += 1
            else:
                sent.append(free + lat)
        fires.append(set(table))
        ready = sent
    done, last, tables = [0, 0, 0], [0, 0], []
    k = 0
    for units, points in ((blocks, 4), (tiles, 2)):
        starts, codes = [], []
        for _ in range(units):
            starts.append(done[0] + 64 * done[1] + 4096 * done[2] + 262144 * last[0] + 524288 * last[1])
            code = 0
            for p in range(points):
                f = [int(k in fire) for fire in fires]
                code += sum(v * 2 ** (3 * p + step) for step, v in enumerate(f))
                done = [a + b for a, b in zip(done, f)]
                last = f[:2]
                k += 1
            codes.append(code)
        tables.append((tuple(starts), tuple(codes), points))
    return tables[0], tables[1], (tuple(done), last[0], last[1])


def copy_kernel(*refs):
    n = len(refs) // 4
    pieces = []
    for src, dst, buf, sem in zip(refs[:n], refs[n:2 * n], refs[2 * n:3 * n], refs[3 * n:]):
        count = sem.shape[1]
        rows = src.shape[0] // count
        for p in range(count):
            part = pl.ds(p * rows, rows)
            pieces.append((pltpu.make_async_copy(src.at[part], buf.at[part], sem.at[0, p]), pltpu.make_async_copy(buf.at[part], dst.at[part], sem.at[1, p])))
    for load, _ in pieces:
        load.start()
    for load, store in pieces:
        load.wait()
        store.start()
    for _, store in pieces:
        store.wait()


def copy_out(arrays):
    any_spec = pl.BlockSpec(memory_space=pl.ANY)
    counts = [2 ** max(0, (a.size // (512 * 1024)).bit_length() - 1) for a in arrays]
    return pl.pallas_call(
        copy_kernel, name="results",
        out_shape=[jax.ShapeDtypeStruct(a.shape, a.dtype) for a in arrays],
        in_specs=[any_spec] * len(arrays), out_specs=[any_spec] * len(arrays),
        scratch_shapes=[pltpu.VMEM(a.shape, a.dtype) for a in arrays] + [pltpu.SemaphoreType.DMA((2, c)) for c in counts],
        compiler_params=pltpu.CompilerParams(vmem_limit_bytes=67043328))(*arrays)


def rope_tables(blocks, head_dim):
    rot = head_dim // 4
    half = rot // 2
    inv_freq = np.power(np.float32(10000.0), (-2.0 * np.arange(half, dtype=np.float32) / rot).astype(np.float32)).astype(np.float64)
    freq = np.zeros((1, 128))
    freq[0, :half], freq[0, half:rot] = -inv_freq, inv_freq
    at = np.arange(blocks)[:, None] * ROWS * freq
    off = np.arange(ROWS)[:, None] * freq
    return [np.asarray(t, np.float32) for t in (np.cos(at), np.sin(at), np.cos(off), np.sin(off))]


def solution(mesh):
    def device_step(resid_x, ln_mean, ln_rstd, ln_gain, grad_y, w_qkv, w_out, w_up, w_down):
        T, D = resid_x.shape
        F = w_up.shape[1]
        H = w_out.shape[1]
        NB = T // ROWS
        HALF = ROWS // 2
        C = min(1024, T)
        tabs = [jnp.asarray(t) for t in rope_tables(NB, H)]
        small = jnp.concatenate([ln_mean, ln_rstd, ln_gain.astype(F32)]).reshape(2 * NB + D // ROWS, ROWS)
        any_spec = pl.BlockSpec(memory_space=pl.ANY)
        vmem = pl.BlockSpec(memory_space=pltpu.VMEM)
        sds = lambda *s: jax.ShapeDtypeStruct(s, BF16)
        outs = pl.pallas_call(
            functools.partial(layer_kernel, (T, D, F, H, C), service_plan(NB, D // H + F // H + 1)),
            name="layer_backward",
            out_shape=[sds(T, D), sds(D, 3 * H), sds(H, D), sds(D, F), sds(F, D),
                       sds(T, D), sds(T, F), sds(T, F), sds(T, 3 * H), sds(T, H), sds(2 * NB, HALF // 2, D), sds(2 * NB, HALF // 2, D)],
            in_specs=[any_spec, any_spec] + [vmem] * 5 + [any_spec, any_spec, any_spec, any_spec],
            out_specs=[any_spec] * 12,
            scratch_shapes=[
                pltpu.VMEM((1, D), F32), pltpu.VMEM((2 * NB, HALF // 2, D), BF16), pltpu.VMEM((ROWS, D), BF16), pltpu.VMEM((2, HALF, D), BF16),
                *[pltpu.VMEM((HALF // 2, D), BF16)] * 4,
                pltpu.SemaphoreType.DMA((2,)), pltpu.SemaphoreType.DMA((2,))]
            + [pltpu.SemaphoreType.DMA((2 * NB,))] * 8
            + [pltpu.SemaphoreType.DMA((4,)), pltpu.SemaphoreType.DMA((2, 2)), pltpu.SemaphoreType.DMA((4,)), pltpu.SemaphoreType.DMA((4, 2)),
               pltpu.SemaphoreType.DMA((3, 2))],
            compiler_params=pltpu.CompilerParams(collective_id=0, has_side_effects=True, vmem_limit_bytes=67043328),
        )(resid_x, grad_y, small, *tabs, w_qkv, w_out.reshape(H, D), w_up, w_down)
        grad_x, grad_w_qkv, grad_w_out, grad_w_up, grad_w_down = copy_out(outs[:5])
        return grad_x, grad_w_qkv, grad_w_out.reshape(1, H, D), grad_w_up, grad_w_down

    in_specs = (P("data", None), P("data"), P("data"), P(None), P("data", None), P(None, "model"), P("model", None, None), P(None, "model"), P("model", None))
    out_specs = (P("data", None), P("data", "model"), P(("data", "model"), None, None), P("data", "model"), P(("data", "model"), None))
    return jax.shard_map(device_step, mesh=mesh, in_specs=in_specs, out_specs=out_specs, check_vma=False)
```
